16 devices in a mesh: dp: 4 (over z, y), tp: 4 (over x, core).
Axes of the slice: x: 2, y: 2, z: 2, core: 2. Of those that a mesh axis runs over, the one named last changes fastest.
Arguments:
- x_in: bfloat16 [16, 64, 5120], P('dp'), parts along dimension 0
- start_pos: int32 [16], P('dp'), parts along dimension 0
- kv_state: float32 [16, 20, 256, 512], P('dp', 'tp'), parts along dimension 0
- ln1_gain: float32 [5120], replicated
- ln1_bias: float32 [5120], replicated
- w_q: bfloat16 [5120, 5120], P(None, 'tp')
- w_k: bfloat16 [5120, 5120], P(None, 'tp')
- w_v: bfloat16 [5120, 10240], P(None, 'tp')
- w_g: bfloat16 [5120, 10240], P(None, 'tp')
- w_o: bfloat16 [10240, 5120], P('tp')
- ln2_gain: float32 [5120], replicated
- ln2_bias: float32 [5120], replicated
- w_up: bfloat16 [5120, 10240], P(None, 'tp')
- w_down: bfloat16 [10240, 5120], P('tp')
Outputs:
- output 1: bfloat16 [16, 64, 5120], P('dp'), parts along dimension 0
- output 2: float32 [16, 20, 256, 512], P('dp', 'tp'), parts along dimension 0
There are 4 independent parts. The reference program is written for one: setup_inputs(seed, part) draws one part's arguments, and reference() takes and returns one part's arrays. A program takes and returns all parts, laid end to end along the dimension named above; an argument that names none is the same for every part.
All inputs are finite; a program needn't handle non-finite values.
Results may differ from the reference program's by a relative error of at most 0.0131123.
Values are sent between devices in bfloat16 or wider.
A program may use at most 1 GiB of HBM per device.

```python
import jax
import jax.numpy as jnp
from jax import lax

BATCH_SEQS = 4
CHUNK_LEN = 64
D_MODEL = 5120
NUM_HEADS = 20
FFN_DIM = 10240
POS_LIMIT = 4096

KEY_DIM = D_MODEL // NUM_HEADS
VAL_DIM = 2 * KEY_DIM
HALF_DIM = KEY_DIM // 2
NORM_EPS = 1e-5
GROUP_EPS = 1e-6
ROPE_BASE = 10000.0


def head_log_decay():
    head_ids = jnp.arange(NUM_HEADS).astype(jnp.float32)
    return jnp.log1p(-jnp.exp2(-5.0 - head_ids))


def setup_inputs(seed: int = 0, part: int = 0) -> dict:
    base_key = jax.random.key(seed)
    weight_keys = jax.random.split(base_key, 12)
    part_keys = jax.random.split(jax.random.fold_in(weight_keys[11], part), 3)

    def normal_weight(key_index, arr_shape, fan_in):
        raw_draw = jax.random.normal(weight_keys[key_index], arr_shape, jnp.float32)
        return (raw_draw * fan_in ** -0.5).astype(jnp.bfloat16)

    x_in = jax.random.normal(part_keys[0], (BATCH_SEQS, CHUNK_LEN, D_MODEL), jnp.float32).astype(jnp.bfloat16)
    start_pos = jax.random.randint(part_keys[1], (BATCH_SEQS,), 64, POS_LIMIT, dtype=jnp.int32)
    log_gamma = head_log_decay()
    decayed_var = jnp.expm1(2.0 * start_pos.astype(jnp.float32)[:, None] * log_gamma[None, :]) / jnp.expm1(2.0 * log_gamma)[None, :]
    state_draw = jax.random.normal(part_keys[2], (BATCH_SEQS, NUM_HEADS, KEY_DIM, VAL_DIM), jnp.float32)
    kv_state = state_draw * jnp.sqrt(decayed_var / KEY_DIM)[:, :, None, None]
    return {
        'x_in': x_in,
        'start_pos': start_pos,
        'kv_state': kv_state,
        'ln1_gain': 1.0 + 0.3 * jax.random.normal(weight_keys[0], (D_MODEL,), jnp.float32),
        'ln1_bias': 0.3 * jax.random.normal(weight_keys[1], (D_MODEL,), jnp.float32),
        'w_q': normal_weight(2, (D_MODEL, D_MODEL), D_MODEL),
        'w_k': normal_weight(3, (D_MODEL, D_MODEL), D_MODEL),
        'w_v': normal_weight(4, (D_MODEL, 2 * D_MODEL), D_MODEL),
        'w_g': normal_weight(5, (D_MODEL, 2 * D_MODEL), D_MODEL),
        'w_o': normal_weight(6, (2 * D_MODEL, D_MODEL), 2 * D_MODEL),
        'ln2_gain': 1.0 + 0.3 * jax.random.normal(weight_keys[7], (D_MODEL,), jnp.float32),
        'ln2_bias': 0.3 * jax.random.normal(weight_keys[8], (D_MODEL,), jnp.float32),
        'w_up': normal_weight(9, (D_MODEL, FFN_DIM), D_MODEL),
        'w_down': normal_weight(10, (FFN_DIM, D_MODEL), FFN_DIM),
    }


def layer_norm(x_f32, norm_gain, norm_bias):
    row_mean = jnp.mean(x_f32, axis=-1, keepdims=True)
    centered = x_f32 - row_mean
    variance = jnp.mean(centered * centered, axis=-1, keepdims=True)
    return centered * lax.rsqrt(variance + NORM_EPS) * norm_gain + norm_bias


def rotate_half(head_vecs, cos_t, sin_t):
    first_half = head_vecs[..., :HALF_DIM]
    second_half = head_vecs[..., HALF_DIM:]
    return jnp.concatenate([first_half * cos_t - second_half * sin_t, second_half * cos_t + first_half * sin_t], axis=-1)


def reference(x_in, start_pos, kv_state, ln1_gain, ln1_bias, w_q, w_k, w_v, w_g, w_o, ln2_gain, ln2_bias, w_up, w_down):
    log_gamma = head_log_decay()
    step_ids = jnp.arange(CHUNK_LEN)
    step_gap = step_ids[:, None] - step_ids[None, :]
    inner_decay = jnp.where(step_gap[None] >= 0, jnp.exp(jnp.maximum(step_gap, 0).astype(jnp.float32)[None] * log_gamma[:, None, None]), 0.0)
    query_decay = jnp.exp((step_ids + 1).astype(jnp.float32)[:, None] * log_gamma[None, :])
    key_decay = jnp.exp((CHUNK_LEN - 1 - step_ids).astype(jnp.float32)[:, None] * log_gamma[None, :])
    state_decay = jnp.exp(CHUNK_LEN * log_gamma)
    inv_freq = jnp.power(ROPE_BASE, -jnp.arange(HALF_DIM).astype(jnp.float32) / HALF_DIM)

    def one_sequence(packed):
        tokens, first_pos, old_state = packed
        x_f32 = tokens.astype(jnp.float32)
        h_one = layer_norm(x_f32, ln1_gain, ln1_bias).astype(jnp.bfloat16)
        angles = (first_pos + step_ids).astype(jnp.float32)[:, None] * inv_freq[None, :]
        cos_t = jnp.cos(angles)[:, None, :]
        sin_t = jnp.sin(angles)[:, None, :]
        q_raw = jnp.dot(h_one, w_q, preferred_element_type=jnp.float32).reshape(CHUNK_LEN, NUM_HEADS, KEY_DIM)
        k_raw = jnp.dot(h_one, w_k, preferred_element_type=jnp.float32).reshape(CHUNK_LEN, NUM_HEADS, KEY_DIM)
        queries = rotate_half(q_raw, cos_t, sin_t).astype(jnp.bfloat16).astype(jnp.float32)
        keys = (rotate_half(k_raw, cos_t, sin_t) * KEY_DIM ** -0.5).astype(jnp.bfloat16).astype(jnp.float32)
        values = jnp.dot(h_one, w_v, preferred_element_type=jnp.float32).astype(jnp.bfloat16).astype(jnp.float32).reshape(CHUNK_LEN, NUM_HEADS, VAL_DIM)
        gates = jnp.dot(h_one, w_g, preferred_element_type=jnp.float32).reshape(CHUNK_LEN, NUM_HEADS, VAL_DIM)
        scores = jnp.einsum('chk,jhk->hcj', queries, keys) * inner_decay
        retained = jnp.einsum('hcj,jhe->che', scores, values) + jnp.einsum('chk,hke->che', queries, old_state) * query_decay[:, :, None]
        row_mean = jnp.mean(retained, axis=-1, keepdims=True)
        centered = retained - row_mean
        variance = jnp.mean(centered * centered, axis=-1, keepdims=True)
        normed = centered * lax.rsqrt(variance + GROUP_EPS)
        mixed = (jax.nn.silu(gates) * normed).astype(jnp.bfloat16).reshape(CHUNK_LEN, 2 * D_MODEL)
        attn_out = jnp.dot(mixed, w_o, preferred_element_type=jnp.float32).astype(jnp.bfloat16)
        x_mid = (x_f32 + attn_out.astype(jnp.float32)).astype(jnp.bfloat16)
        h_two = layer_norm(x_mid.astype(jnp.float32), ln2_gain, ln2_bias).astype(jnp.bfloat16)
        activated = jax.nn.gelu(jnp.dot(h_two, w_up, preferred_element_type=jnp.float32), approximate=False).astype(jnp.bfloat16)
        ffn_out = jnp.dot(activated, w_down, preferred_element_type=jnp.float32).astype(jnp.bfloat16)
        x_out = (x_mid.astype(jnp.float32) + ffn_out.astype(jnp.float32)).astype(jnp.bfloat16)
        new_state = state_decay[:, None, None] * old_state + jnp.einsum('jhk,jhe->hke', keys * key_decay[:, :, None], values)
        return x_out, new_state

    x_out, state_out = lax.map(one_sequence, (x_in, start_pos, kv_state))
    return (x_out, state_out)
```

```python
import numpy as np
import jax
import jax.numpy as jnp
from jax import lax
from jax.experimental import pallas as pl
from jax.experimental.pallas import tpu as pltpu
from jax.sharding import PartitionSpec as P

NORM_EPS = 1e-5
GROUP_EPS = 1e-6
ROPE_BASE = 10000.0
BF = jnp.bfloat16
F32 = jnp.float32
MESH = pl.DeviceIdType.MESH


def layer_norm(x_f32, norm_gain, norm_bias):
    row_mean = jnp.mean(x_f32, axis=-1, keepdims=True)
    centered = x_f32 - row_mean
    variance = jnp.mean(centered * centered, axis=-1, keepdims=True)
    return centered * lax.rsqrt(variance + NORM_EPS) * norm_gain + norm_bias


def rope_tables(first_pos, chunk_len, key_dim):
    half_dim = key_dim // 2
    inv_freq = jnp.power(ROPE_BASE, -jnp.arange(half_dim).astype(F32) / half_dim)
    positions = (first_pos[:, None] + jnp.arange(chunk_len)[None, :]).astype(F32)
    angles = (positions[:, :, None] * inv_freq).reshape(-1, half_dim)
    return jnp.cos(angles), jnp.sin(angles)


def split2(val):
    high = val.astype(BF)
    return high, (val - high.astype(F32)).astype(BF)


def dot(lhs, rhs):
    return jnp.dot(lhs, rhs, preferred_element_type=F32)


def mix_kernel(lg_ref, x_hbm, cos_ref, sin_ref, g_ref, b_ref, wq, wk, wv, wg, s_hbm, z_hbm, so_hbm,
               xb, hb, wb, sb, sob, qb, kb, vb, gb, zb, xsem, wsem, ssem, sosem, zsem):
    heads = wq.shape[1] // 256
    nseq = s_hbm.shape[0]
    clen = x_hbm.shape[0] // nseq
    first_head = lax.axis_index('tp') * heads

    def wcopy(head, i):
        if i == 0:
            src = wq.at[:, pl.ds(pl.multiple_of(head * 256, 256), 256)]
        elif i == 1:
            src = wk.at[:, pl.ds(pl.multiple_of(head * 256, 256), 256)]
        elif i < 4:
            src = wv.at[:, pl.ds(pl.multiple_of(head * 512 + (i - 2) * 256, 256), 256)]
        else:
            src = wg.at[:, pl.ds(pl.multiple_of(head * 512 + (i - 4) * 256, 256), 256)]
        return pltpu.make_async_copy(src, wb.at[i], wsem.at[i])

    def scopy(head):
        slot = lax.rem(head, 2)
        return pltpu.make_async_copy(s_hbm.at[:, head], sb.at[slot], ssem.at[slot])

    def socopy(head):
        slot = lax.rem(head, 2)
        return pltpu.make_async_copy(sob.at[slot], so_hbm.at[:, head], sosem.at[slot])

    def zcopy(head):
        slot = lax.rem(head, 2)
        return pltpu.make_async_copy(zb.at[slot], z_hbm.at[:, pl.ds(pl.multiple_of(head * 512, 512), 512)], zsem.at[slot])

    xcopy = pltpu.make_async_copy(x_hbm, xb, xsem)
    xcopy.start()
    for i in range(3):
        wcopy(0, i).start()
    scopy(0).start()
    for i in range(3, 6):
        wcopy(0, i).start()
    xcopy.wait()

    def ln_rows(r, carry):
        rows = pl.ds(pl.multiple_of(r * 16, 16), 16)
        hb[rows, :] = layer_norm(xb[rows, :].astype(F32), g_ref[...], b_ref[...]).astype(BF)
        return carry
    lax.fori_loop(0, xb.shape[0] // 16, ln_rows, 0)

    step_i = lax.broadcasted_iota(jnp.int32, (clen, clen), 0)
    step_j = lax.broadcasted_iota(jnp.int32, (clen, clen), 1)
    gap = step_i - step_j
    tok_q = lax.broadcasted_iota(jnp.int32, (clen, 512), 0).astype(F32)
    tok_k = lax.broadcasted_iota(jnp.int32, (clen, 256), 0).astype(F32)

    def head_body(head, carry):
        def proj(i):
            wcopy(head, i).wait()
            res = dot(hb[...], wb[i])

            @pl.when(head + 1 < heads)
            def _():
                wcopy(head + 1, i).start()
            return res

        @pl.when(head + 1 < heads)
        def _():
            scopy(head + 1).start()

        cos_t = cos_ref[...]
        sin_t = sin_ref[...]
        res = proj(0)
        qb[:, :128] = (res[:, :128] * cos_t - res[:, 128:] * sin_t).astype(BF)
        qb[:, 128:] = (res[:, 128:] * cos_t + res[:, :128] * sin_t).astype(BF)
        res = proj(1)
        kb[:, :128] = ((res[:, :128] * cos_t - res[:, 128:] * sin_t) * 0.0625).astype(BF)
        kb[:, 128:] = ((res[:, 128:] * cos_t + res[:, :128] * sin_t) * 0.0625).astype(BF)
        vb[:, :256] = proj(2).astype(BF)
        vb[:, 256:] = proj(3).astype(BF)
        gb[:, :256] = proj(4)
        gb[:, 256:] = proj(5)

        log_g = lg_ref[first_head + head]
        inner_decay = jnp.where(gap >= 0, jnp.exp(jnp.maximum(gap, 0).astype(F32) * log_g), 0.0)
        query_decay = jnp.exp((tok_q + 1.0) * log_g)
        key_decay = jnp.exp((clen - 1.0 - tok_k) * log_g)
        state_decay = jnp.exp(jnp.full((1, 512), clen, F32) * log_g)
        slot = lax.rem(head, 2)
        scopy(head).wait()

        @pl.when(head >= 2)
        def _():
            socopy(head - 2).wait()
            zcopy(head - 2).wait()

        for s in range(nseq):
            rows = slice(s * clen, (s + 1) * clen)
            q, k, v = qb[rows, :], kb[rows, :], vb[rows, :]
            scores = lax.dot_general(q, k, (((1,), (1,)), ((), ())), preferred_element_type=F32) * inner_decay
            sc_hi, sc_lo = split2(scores)
            state = sb[slot, s]
            st_hi, st_lo = split2(state)
            out = dot(sc_hi, v) + dot(sc_lo, v) + (dot(q, st_hi) + dot(q, st_lo)) * query_decay
            mean = jnp.mean(out, axis=-1, keepdims=True)
            cent = out - mean
            var = jnp.mean(cent * cent, axis=-1, keepdims=True)
            gates = gb[rows, :]
            zb[slot, rows, :] = (gates * jax.nn.sigmoid(gates) * (cent * lax.rsqrt(var + GROUP_EPS))).astype(BF)
            kd_hi, kd_lo = split2(k.astype(F32) * key_decay)
            tdot = lambda a: lax.dot_general(a, v, (((0,), (0,)), ((), ())), preferred_element_type=F32)
            sob[slot, s] = state * state_decay + (tdot(kd_hi) + tdot(kd_lo))
        socopy(head).start()
        zcopy(head).start()
        return carry

    lax.fori_loop(0, heads, head_body, 0)
    for head in (heads - 2, heads - 1):
        socopy(head).wait()
        zcopy(head).wait()


def mix_call(x2d, cos_t, sin_t, gain, bias, w_q, w_k, w_v, w_g, state, log_gammas):
    rows, d_model = x2d.shape
    nseq, heads = state.shape[:2]
    anyspec = pl.BlockSpec(memory_space=pl.ANY)
    vspec = pl.BlockSpec(memory_space=pltpu.VMEM)
    return pl.pallas_call(
        mix_kernel,
        out_shape=(jax.ShapeDtypeStruct((rows, heads * 512), BF), jax.ShapeDtypeStruct(state.shape, F32)),
        in_specs=[pl.BlockSpec(memory_space=pltpu.SMEM), anyspec, vspec, vspec, vspec, vspec] + [anyspec] * 5,
        out_specs=(anyspec, anyspec),
        scratch_shapes=[
            pltpu.VMEM((rows, d_model), BF), pltpu.VMEM((rows, d_model), BF),
            pltpu.VMEM((6, d_model, 256), BF),
            pltpu.VMEM((2, nseq, 256, 512), F32), pltpu.VMEM((2, nseq, 256, 512), F32),
            pltpu.VMEM((rows, 256), BF), pltpu.VMEM((rows, 256), BF), pltpu.VMEM((rows, 512), BF),
            pltpu.VMEM((rows, 512), F32), pltpu.VMEM((2, rows, 512), BF),
            pltpu.SemaphoreType.DMA, pltpu.SemaphoreType.DMA((6,)), pltpu.SemaphoreType.DMA((2,)),
            pltpu.SemaphoreType.DMA((2,)), pltpu.SemaphoreType.DMA((2,)),
        ],
        compiler_params=pltpu.CompilerParams(vmem_limit_bytes=60 * 1024 * 1024),
        cost_estimate=pl.CostEstimate(flops=21_000_000_000, bytes_accessed=102_000_000, transcendentals=0),
        name='mix',
    )(log_gammas, x2d, cos_t, sin_t, gain, bias, w_q, w_k, w_v, w_g, state)


TN = 512


def ffn_kernel(z_hbm, x_hbm, g_ref, b_ref, wo, wup, wdn, o_hbm,
               zb, wa, wbb, ub, drv, xrv, h2, x1,
               zsem, x1sem, wosem, wupsem, wdnsem, ds_sem, dr_sem, xs_sem, xr_sem, hs_sem, hr_sem, ol_sem, os_sem, or_sem):
    tp = lax.axis_index('tp')
    core = lax.rem(tp, 2)
    sib = {'tp': tp + 1 - 2 * core}
    nbr = {'tp': lax.rem(tp + 2, 4)}
    nt = wo.shape[1] // TN
    ku = wup.shape[1] // 256
    hrows = ub.shape[2]

    def wo_copy(n):
        return pltpu.make_async_copy(wo.at[:, pl.ds(pl.multiple_of(n * TN, TN), TN)], wbb.at[n], wosem.at[n])

    def wdn_copy(n):
        return pltpu.make_async_copy(wdn.at[:, pl.ds(pl.multiple_of(n * TN, TN), TN)], wbb.at[n], wdnsem.at[n])

    def wup_copy(n):
        return pltpu.make_async_copy(wup.at[:, pl.ds(pl.multiple_of(n * 256, 256), 256)], wa.at[n], wupsem.at[n])

    def x1_copy(c):
        src = x_hbm.at[pl.ds(pl.multiple_of((c * 2 + core) * hrows, hrows), hrows)]
        return pltpu.make_async_copy(src, x1.at[c], x1sem.at[c])

    zcopy = pltpu.make_async_copy(z_hbm, zb, zsem)
    zcopy.start()

    def start_wo(n, carry):
        wo_copy(n).start()
        return carry
    lax.fori_loop(0, nt, start_wo, 0)
    x1_copy(0).start()
    x1_copy(1).start()

    def start_wup(n, carry):
        wup_copy(n).start()
        return carry
    lax.fori_loop(0, ku, start_wup, 0)

    barrier = pltpu.get_barrier_semaphore()
    pl.semaphore_signal(barrier, inc=1, device_id=sib, device_id_type=MESH)
    pl.semaphore_signal(barrier, inc=1, device_id=nbr, device_id_type=MESH)
    pl.semaphore_wait(barrier, 2)

    def d_copy(r, c, n):
        return pltpu.make_async_remote_copy(
            src_ref=ub.at[c * 2 + 1 - core, n], dst_ref=drv.at[c, n], send_sem=ds_sem.at[r, c, n], recv_sem=dr_sem.at[r, c, n],
            device_id=sib, device_id_type=MESH)

    def x_copy(r, c, n):
        return pltpu.make_async_remote_copy(
            src_ref=ub.at[c * 2 + core, n], dst_ref=xrv.at[r, c, n], send_sem=xs_sem.at[r, c, n], recv_sem=xr_sem.at[r, c, n],
            device_id=nbr, device_id_type=MESH)

    def forward(r, c, n):
        d_copy(r, c, n).wait_recv()
        own = ub[c * 2 + core, n].astype(F32)
        ub[c * 2 + core, n] = (own + drv[c, n].astype(F32)).astype(BF)
        x_copy(r, c, n).start()

    lag = 2
    zcopy.wait()

    def wo_step(n, carry):
        wo_copy(n).wait()
        res = dot(zb[...], wbb[n]).astype(BF)
        for j in range(4):
            ub[j, n] = res[j * hrows:(j + 1) * hrows]
        d_copy(0, 0, n).start()
        d_copy(0, 1, n).start()
        wdn_copy(n).start()

        @pl.when(n >= lag)
        def _():
            forward(0, 0, n - lag)
        return carry
    lax.fori_loop(0, nt, wo_step, 0)
    for n in range(nt - lag, nt):
        forward(0, 0, n)

    def fwd1(n, carry):
        forward(0, 1, n)
        return carry
    lax.fori_loop(0, nt, fwd1, 0)

    def h_copy(c):
        own = h2.at[c, pl.ds(pl.multiple_of(core * hrows, hrows), hrows)]
        return pltpu.make_async_remote_copy(src_ref=own, dst_ref=own, send_sem=hs_sem.at[c], recv_sem=hr_sem.at[c],
                                            device_id=sib, device_id_type=MESH)

    def chunk(c):
        x1_copy(c).wait()
        for n in range(nt):
            x_copy(0, c, n).wait_recv()

        def ln_rows(r, carry):
            rows = pl.ds(pl.multiple_of(r * 16, 16), 16)
            total = jnp.concatenate(
                [(ub[c * 2 + core, n, rows, :].astype(F32) + xrv[0, c, n, rows, :].astype(F32)).astype(BF) for n in range(nt)], axis=-1)
            mid = (x1[c, rows, :].astype(F32) + total.astype(F32)).astype(BF)
            x1[c, rows, :] = mid
            hrow = pl.ds(pl.multiple_of(core * hrows + r * 16, 16), 16)
            h2[c, hrow, :] = layer_norm(mid.astype(F32), g_ref[...], b_ref[...]).astype(BF)
            return carry
        lax.fori_loop(0, hrows // 16, ln_rows, 0)
        h_copy(c).start()

        def drain(n, carry):
            d_copy(0, c, n).wait_send()
            x_copy(0, c, n).wait_send()
            return carry
        lax.fori_loop(0, nt, drain, 0)
        h_copy(c).wait_recv()

        def up_step(n, carry):
            if c == 0:
                wup_copy(n).wait()
            res = dot(h2[c], wa[n])
            res = 0.5 * res * (1.0 + lax.erf(res * (0.5 ** 0.5)))
            zb[c * 2 * hrows:(c + 1) * 2 * hrows, pl.ds(pl.multiple_of(n * 256, 256), 256)] = res.astype(BF)
            return carry
        lax.fori_loop(0, ku, up_step, 0)

        def down_step(n, carry):
            if c == 0:
                wdn_copy(n).wait()
            res = dot(zb[c * 2 * hrows:(c + 1) * 2 * hrows, :], wbb[n]).astype(BF)
            for j in range(2):
                ub[c * 2 + j, n] = res[j * hrows:(j + 1) * hrows]
            d_copy(1, c, n).start()

            @pl.when(n >= lag)
            def _():
                forward(1, c, n - lag)
            return carry
        lax.fori_loop(0, nt, down_step, 0)
        for n in range(nt - lag, nt):
            forward(1, c, n)

    chunk(0)
    chunk(1)

    def o_copies(c, n):
        src = x1.at[c, :, pl.ds(pl.multiple_of(n * TN, TN), TN)]
        dst = o_hbm.at[pl.ds(pl.multiple_of((c * 2 + core) * hrows, hrows), hrows), pl.ds(pl.multiple_of(n * TN, TN), TN)]
        local = pltpu.make_async_copy(src, dst, ol_sem.at[c, n])
        remote = pltpu.make_async_remote_copy(src_ref=src, dst_ref=dst, send_sem=os_sem.at[c, n], recv_sem=or_sem.at[c, n],
                                              device_id=sib, device_id_type=MESH)
        return local, remote

    for c in range(2):
        def out_step(n, carry):
            x_copy(1, c, n).wait_recv()
            cols = pl.ds(pl.multiple_of(n * TN, TN), TN)
            total = (ub[c * 2 + core, n].astype(F32) + xrv[1, c, n].astype(F32)).astype(BF)
            x1[c, :, cols] = (x1[c, :, cols].astype(F32) + total.astype(F32)).astype(BF)
            local, remote = o_copies(c, n)
            remote.start()
            local.start()
            return carry
        lax.fori_loop(0, nt, out_step, 0)
    for c in range(2):
        h_copy(c).wait_send()

        def fin(n, carry):
            d_copy(1, c, n).wait_send()
            x_copy(1, c, n).wait_send()
            local, remote = o_copies(c, n)
            local.wait()
            remote.wait_send()
            remote.wait_recv()
            return carry
        lax.fori_loop(0, nt, fin, 0)


def ffn_call(z2d, x2d, gain, bias, w_o, w_up, w_down):
    rows, d_model = x2d.shape
    width = z2d.shape[1]
    fdim = w_up.shape[1]
    nt = d_model // TN
    ku = fdim // 256
    hr = rows // 4
    anyspec = pl.BlockSpec(memory_space=pl.ANY)
    vspec = pl.BlockSpec(memory_space=pltpu.VMEM)
    dma = pltpu.SemaphoreType.DMA
    return pl.pallas_call(
        ffn_kernel,
        out_shape=jax.ShapeDtypeStruct((rows, d_model), BF),
        in_specs=[anyspec, anyspec, vspec, vspec, anyspec, anyspec, anyspec],
        out_specs=anyspec,
        scratch_shapes=[
            pltpu.VMEM((rows, width), BF),
            pltpu.VMEM((ku, d_model, 256), BF),
            pltpu.VMEM((nt, width, TN), BF),
            pltpu.VMEM((4, nt, hr, TN), BF),
            pltpu.VMEM((2, nt, hr, TN), BF),
            pltpu.VMEM((2, 2, nt, hr, TN), BF),
            pltpu.VMEM((2, 2 * hr, d_model), BF),
            pltpu.VMEM((2, hr, d_model), BF),
            dma, dma((2,)), dma((nt,)), dma((ku,)), dma((nt,)),
            dma((2, 2, nt)), dma((2, 2, nt)), dma((2, 2, nt)), dma((2, 2, nt)), dma((2,)), dma((2,)),
            dma((2, nt)), dma((2, nt)), dma((2, nt)),
        ],
        compiler_params=pltpu.CompilerParams(collective_id=0, has_side_effects=True, vmem_limit_bytes=67043328),
        cost_estimate=pl.CostEstimate(flops=20_000_000_000, bytes_accessed=85_000_000, transcendentals=0),
        name='ffn',
    )(z2d, x2d, gain, bias, w_o, w_up, w_down)


def solution(mesh):
    def local_layer(x_in, start_pos, kv_state, ln1_gain, ln1_bias, w_q, w_k, w_v, w_g, w_o, ln2_gain, ln2_bias, w_up, w_down):
        nseq, clen, d_model = x_in.shape
        x2d = x_in.reshape(nseq * clen, d_model)
        cos_t, sin_t = rope_tables(start_pos, clen, kv_state.shape[2])
        num_heads = kv_state.shape[1] * mesh.shape['tp']
        log_gammas = jnp.asarray(np.log1p(-np.exp2(-5.0 - np.arange(num_heads))).astype(np.float32))
        z2d, new_state = mix_call(x2d, cos_t, sin_t, ln1_gain.reshape(1, -1), ln1_bias.reshape(1, -1),
                                  w_q, w_k, w_v, w_g, kv_state, log_gammas)
        out = ffn_call(z2d, x2d, ln2_gain.reshape(1, -1), ln2_bias.reshape(1, -1), w_o, w_up, w_down)
        return out.reshape(x_in.shape), new_state

    in_specs = (P('dp', None, None), P('dp'), P('dp', 'tp', None, None), P(), P(), P(None, 'tp'), P(None, 'tp'), P(None, 'tp'), P(None, 'tp'), P('tp', None), P(), P(), P(None, 'tp'), P('tp', None))
    out_specs = (P('dp', None, None), P('dp', 'tp', None, None))
    return jax.shard_map(local_layer, mesh=mesh, in_specs=in_specs, out_specs=out_specs, check_vma=False)
```

```python
import numpy as np
import jax
import jax.numpy as jnp
from jax import lax
from jax.experimental import pallas as pl
from jax.experimental.pallas import tpu as pltpu
from jax.sharding import PartitionSpec as P

NORM_EPS = 1e-5
GROUP_EPS = 1e-6
ROPE_BASE = 10000.0
BF = jnp.bfloat16
F32 = jnp.float32
MESH = pl.DeviceIdType.MESH


def layer_norm(x_f32, norm_gain, norm_bias):
    row_mean = jnp.mean(x_f32, axis=-1, keepdims=True)
    centered = x_f32 - row_mean
    variance = jnp.mean(centered * centered, axis=-1, keepdims=True)
    return centered * lax.rsqrt(variance + NORM_EPS) * norm_gain + norm_bias


def rope_tables(first_pos, chunk_len, key_dim):
    half_dim = key_dim // 2
    inv_freq = jnp.power(ROPE_BASE, -jnp.arange(half_dim).astype(F32) / half_dim)
    positions = (first_pos[:, None] + jnp.arange(chunk_len)[None, :]).astype(F32)
    angles = (positions[:, :, None] * inv_freq).reshape(-1, half_dim)
    return jnp.cos(angles), jnp.sin(angles)


def split2(val):
    high = val.astype(BF)
    return high, (val - high.astype(F32)).astype(BF)


def dot(lhs, rhs):
    return jnp.dot(lhs, rhs, preferred_element_type=F32)


def ln_rows(load, store, g_ref, b_ref, width):
    cols = [slice(c, c + 256) for c in range(0, width, 256)]
    total = load(cols[0])
    for col in cols[1:]:
        total = total + load(col)
    mean = jnp.sum(total, axis=-1, keepdims=True) * (1.0 / width)
    total = None
    for col in cols:
        cent = load(col) - mean
        total = cent * cent if total is None else total + cent * cent
    var = jnp.sum(total, axis=-1, keepdims=True) * (1.0 / width)
    scale = lax.rsqrt(var + NORM_EPS)
    for col in cols:
        store(col, ((load(col) - mean) * scale * g_ref[:, col] + b_ref[:, col]).astype(BF))


def mix_kernel(lg_ref, x_hbm, cos_ref, sin_ref, g_ref, b_ref, wq, wk, wv, wg, s_hbm, z_hbm, so_hbm,
               xb, hb, wb, sb, sob, qb, kb, vb, gb, scb, sth, stl, kdb, ob, zb, xsem, wsem, ssem, sosem, zsem):
    heads = wq.shape[1] // 256
    nseq = s_hbm.shape[0]
    clen = x_hbm.shape[0] // nseq
    first_head = lax.axis_index('tp') * heads

    def wcopy(head, i):
        if i == 0:
            src = wq.at[:, pl.ds(pl.multiple_of(head * 256, 256), 256)]
        elif i == 1:
            src = wk.at[:, pl.ds(pl.multiple_of(head * 256, 256), 256)]
        elif i < 4:
            src = wv.at[:, pl.ds(pl.multiple_of(head * 512 + (i - 2) * 256, 256), 256)]
        else:
            src = wg.at[:, pl.ds(pl.multiple_of(head * 512 + (i - 4) * 256, 256), 256)]
        return pltpu.make_async_copy(src, wb.at[i], wsem.at[i])

    def scopy(head):
        slot = lax.rem(head, 2)
        return pltpu.make_async_copy(s_hbm.at[:, head], sb.at[slot], ssem.at[slot])

    def socopy(head):
        slot = lax.rem(head, 2)
        return pltpu.make_async_copy(sob.at[slot], so_hbm.at[:, head], sosem.at[slot])

    def zcopy(head):
        slot = lax.rem(head, 2)
        return pltpu.make_async_copy(zb.at[slot], z_hbm.at[:, pl.ds(pl.multiple_of(head * 512, 512), 512)], zsem.at[slot])

    def xcopy(s):
        rows = pl.ds(pl.multiple_of(s * clen, clen), clen)
        return pltpu.make_async_copy(x_hbm.at[rows], xb.at[rows], xsem.at[s])

    for s in range(nseq):
        xcopy(s).start()
    for i in range(6):
        wcopy(0, i).start()
    scopy(0).start()
    scopy(1).start()

    def ln_body(s, carry):
        xcopy(s).wait()
        rows = pl.ds(pl.multiple_of(s * clen, clen), clen)

        def store(col, val):
            hb[rows, col] = val
        ln_rows(lambda col: xb[rows, col].astype(F32), store, g_ref, b_ref, xb.shape[1])
        return carry
    lax.fori_loop(0, nseq, ln_body, 0)

    step_i = lax.broadcasted_iota(jnp.int32, (clen, clen), 0)
    step_j = lax.broadcasted_iota(jnp.int32, (clen, clen), 1)
    gap = step_i - step_j
    tok_q = lax.broadcasted_iota(jnp.int32, (clen, 512), 0).astype(F32)
    tok_k = lax.broadcasted_iota(jnp.int32, (clen, 256), 0).astype(F32)

    def proj2(head, i):
        return dot(hb[...], wb[i]), dot(hb[...], wb[i + 1])

    def wait2(head, i):
        wcopy(head, i).wait()
        wcopy(head, i + 1).wait()

    def next2(head, i):
        @pl.when(head + 1 < heads)
        def _():
            wcopy(head + 1, i).start()
            wcopy(head + 1, i + 1).start()

    def proj_qk(head, slot):
        cos_t = cos_ref[...]
        sin_t = sin_ref[...]
        q, k = proj2(head, 0)
        qb[slot, :, :128] = (q[:, :128] * cos_t - q[:, 128:] * sin_t).astype(BF)
        qb[slot, :, 128:] = (q[:, 128:] * cos_t + q[:, :128] * sin_t).astype(BF)
        kb[slot, :, :128] = ((k[:, :128] * cos_t - k[:, 128:] * sin_t) * 0.0625).astype(BF)
        kb[slot, :, 128:] = ((k[:, 128:] * cos_t + k[:, :128] * sin_t) * 0.0625).astype(BF)

    def proj_v(head, slot):
        for half, val in enumerate(proj2(head, 2)):
            val = val.astype(BF)
            for s in range(nseq):
                for copy in range(2):
                    vb[slot, s, copy * clen:(copy + 1) * clen, half * 256:(half + 1) * 256] = val[s * clen:(s + 1) * clen]

    def proj_g(head, slot):
        gb[slot, :, :256], gb[slot, :, 256:] = proj2(head, 4)

    def seq_rows(s):
        return slice(s * clen, (s + 1) * clen)

    def ret_scores(slot):
        return [lax.dot_general(qb[slot, seq_rows(s), :], kb[slot, seq_rows(s), :], (((1,), (1,)), ((), ())),
                                preferred_element_type=F32) for s in range(nseq)]

    def ret_prepare(head, slot, scores):
        log_g = lg_ref[first_head + head]
        inner_decay = jnp.where(gap >= 0, jnp.exp(jnp.maximum(gap, 0).astype(F32) * log_g), 0.0)
        key_decay = jnp.exp((clen - 1.0 - tok_k) * log_g)
        for s in range(nseq):
            sth[s], stl[s] = split2(sb[slot, s])
            kdb[s, :clen], kdb[s, clen:] = split2(kb[slot, seq_rows(s), :].astype(F32) * key_decay)
            high, low = split2(scores[s] * inner_decay)
            scb[s] = jnp.concatenate([high, low], axis=-1)

    def ret_out(head, slot):
        log_g = lg_ref[first_head + head]
        query_decay = jnp.exp((tok_q + 1.0) * log_g)
        state_decay = jnp.exp(jnp.full((1, 512), clen, F32) * log_g)
        for s in range(nseq):
            q = qb[slot, seq_rows(s), :]
            ob[seq_rows(s), :] = dot(scb[s], vb[slot, s]) + (dot(q, sth[s]) + dot(q, stl[s])) * query_decay
            update = lax.dot_general(kdb[s], vb[slot, s], (((0,), (0,)), ((), ())), preferred_element_type=F32)
            sob[slot, s] = sb[slot, s] * state_decay + update

    def ret_gate(slot):
        for s in range(nseq):
            out = ob[seq_rows(s), :]
            mean = jnp.mean(out, axis=-1, keepdims=True)
            cent = out - mean
            var = jnp.mean(cent * cent, axis=-1, keepdims=True)
            gates = gb[slot, seq_rows(s), :]
            zb[slot, seq_rows(s), :] = (gates * jax.nn.sigmoid(gates) * (cent * lax.rsqrt(var + GROUP_EPS))).astype(BF)

    wait2(0, 0)
    proj_qk(0, 0)
    next2(0, 0)
    wait2(0, 2)
    proj_v(0, 0)
    next2(0, 2)
    wait2(0, 4)
    proj_g(0, 0)
    next2(0, 4)

    def head_body(head, carry):
        prev = head - 1
        slot = lax.rem(head, 2)
        old = 1 - slot
        scopy(prev).wait()

        @pl.when(prev >= 2)
        def _():
            socopy(prev - 2).wait()
            zcopy(prev - 2).wait()
        wait2(head, 0)
        scores = ret_scores(old)
        proj_qk(head, slot)
        ret_prepare(prev, old, scores)
        next2(head, 0)
        wait2(head, 2)
        ret_out(prev, old)
        proj_v(head, slot)
        next2(head, 2)
        socopy(prev).start()

        @pl.when(head + 1 < heads)
        def _():
            scopy(head + 1).start()
        wait2(head, 4)
        proj_g(head, slot)
        ret_gate(old)
        next2(head, 4)
        zcopy(prev).start()
        return carry

    lax.fori_loop(1, heads, head_body, 0)
    last = heads - 1
    slot = last % 2
    scopy(last).wait()
    socopy(last - 2).wait()
    zcopy(last - 2).wait()
    ret_prepare(last, slot, ret_scores(slot))
    ret_out(last, slot)
    socopy(last).start()
    ret_gate(slot)
    zcopy(last).start()
    for head in (last - 1, last):
        socopy(head).wait()
        zcopy(head).wait()


def mix_call(x2d, cos_t, sin_t, gain, bias, w_q, w_k, w_v, w_g, state, log_gammas):
    rows, d_model = x2d.shape
    nseq, heads = state.shape[:2]
    clen = rows // nseq
    anyspec = pl.BlockSpec(memory_space=pl.ANY)
    vspec = pl.BlockSpec(memory_space=pltpu.VMEM)
    return pl.pallas_call(
        mix_kernel,
        out_shape=(jax.ShapeDtypeStruct((rows, heads * 512), BF), jax.ShapeDtypeStruct(state.shape, F32)),
        in_specs=[pl.BlockSpec(memory_space=pltpu.SMEM), anyspec, vspec, vspec, vspec, vspec] + [anyspec] * 5,
        out_specs=(anyspec, anyspec),
        scratch_shapes=[
            pltpu.VMEM((rows, d_model), BF), pltpu.VMEM((rows, d_model), BF),
            pltpu.VMEM((6, d_model, 256), BF),
            pltpu.VMEM((2, nseq, 256, 512), F32), pltpu.VMEM((2, nseq, 256, 512), F32),
            pltpu.VMEM((2, rows, 256), BF), pltpu.VMEM((2, rows, 256), BF), pltpu.VMEM((2, nseq, 2 * clen, 512), BF),
            pltpu.VMEM((2, rows, 512), F32),
            pltpu.VMEM((nseq, clen, 2 * clen), BF), pltpu.VMEM((nseq, 256, 512), BF), pltpu.VMEM((nseq, 256, 512), BF),
            pltpu.VMEM((nseq, 2 * clen, 256), BF), pltpu.VMEM((rows, 512), F32), pltpu.VMEM((2, rows, 512), BF),
            pltpu.SemaphoreType.DMA((nseq,)), pltpu.SemaphoreType.DMA((6,)), pltpu.SemaphoreType.DMA((2,)),
            pltpu.SemaphoreType.DMA((2,)), pltpu.SemaphoreType.DMA((2,)),
        ],
        compiler_params=pltpu.CompilerParams(vmem_limit_bytes=60 * 1024 * 1024),
        cost_estimate=pl.CostEstimate(flops=21_000_000_000, bytes_accessed=102_000_000, transcendentals=0),
        name='mix',
    )(log_gammas, x2d, cos_t, sin_t, gain, bias, w_q, w_k, w_v, w_g, state)


TN = 512


def ffn_kernel(z_hbm, x_hbm, g_ref, b_ref, wo, wup, wdn, o_hbm,
               zb, wa, wbb, ub, drv, xrv, h2, x1,
               zsem, x1sem, wosem, wupsem, wdnsem, ds_sem, dr_sem, xs_sem, xr_sem, hs_sem, hr_sem, ol_sem, os_sem, or_sem):
    tp = lax.axis_index('tp')
    core = lax.rem(tp, 2)
    sib = {'tp': tp + 1 - 2 * core}
    nbr = {'tp': lax.rem(tp + 2, 4)}
    nt = wo.shape[1] // TN
    ku = wup.shape[1] // 256
    hrows = ub.shape[2]

    def wo_copy(n):
        return pltpu.make_async_copy(wo.at[:, pl.ds(pl.multiple_of(n * TN, TN), TN)], wbb.at[n], wosem.at[n])

    def wdn_copy(n):
        return pltpu.make_async_copy(wdn.at[:, pl.ds(pl.multiple_of(n * TN, TN), TN)], wbb.at[n], wdnsem.at[n])

    def wup_copy(n):
        return pltpu.make_async_copy(wup.at[:, pl.ds(pl.multiple_of(n * 256, 256), 256)], wa.at[n], wupsem.at[n])

    def x1_copy(c):
        src = x_hbm.at[pl.ds(pl.multiple_of((c * 2 + core) * hrows, hrows), hrows)]
        return pltpu.make_async_copy(src, x1.at[c], x1sem.at[c])

    zcopy = pltpu.make_async_copy(z_hbm, zb, zsem)
    zcopy.start()

    def start_wo(n, carry):
        wo_copy(n).start()
        return carry
    lax.fori_loop(0, nt, start_wo, 0)
    x1_copy(0).start()
    x1_copy(1).start()

    def start_wup(n, carry):
        wup_copy(n).start()
        return carry
    lax.fori_loop(0, ku, start_wup, 0)

    barrier = pltpu.get_barrier_semaphore()
    pl.semaphore_signal(barrier, inc=1, device_id=sib, device_id_type=MESH)
    pl.semaphore_signal(barrier, inc=1, device_id=nbr, device_id_type=MESH)
    pl.semaphore_wait(barrier, 2)

    def d_copy(r, c, n):
        return pltpu.make_async_remote_copy(
            src_ref=ub.at[c * 2 + 1 - core, n], dst_ref=drv.at[c, n], send_sem=ds_sem.at[r, c, n], recv_sem=dr_sem.at[r, c, n],
            device_id=sib, device_id_type=MESH)

    def x_copy(r, c, n):
        return pltpu.make_async_remote_copy(
            src_ref=ub.at[c * 2 + core, n], dst_ref=xrv.at[r, c, n], send_sem=xs_sem.at[r, c, n], recv_sem=xr_sem.at[r, c, n],
            device_id=nbr, device_id_type=MESH)

    def forward(r, c, n):
        d_copy(r, c, n).wait_recv()
        own = ub[c * 2 + core, n].astype(F32)
        ub[c * 2 + core, n] = (own + drv[c, n].astype(F32)).astype(BF)
        x_copy(r, c, n).start()

    lag = 2
    zcopy.wait()

    def wo_step(n, carry):
        wo_copy(n).wait()
        res = dot(zb[...], wbb[n]).astype(BF)
        for j in range(4):
            ub[j, n] = res[j * hrows:(j + 1) * hrows]
        d_copy(0, 0, n).start()
        d_copy(0, 1, n).start()
        wdn_copy(n).start()

        @pl.when(n >= lag)
        def _():
            forward(0, 0, n - lag)
        return carry
    lax.fori_loop(0, nt, wo_step, 0)
    for n in range(nt - lag, nt):
        forward(0, 0, n)

    def fwd1(n, carry):
        forward(0, 1, n)
        return carry
    lax.fori_loop(0, nt, fwd1, 0)

    def h_copy(c):
        own = h2.at[c, pl.ds(pl.multiple_of(core * hrows, hrows), hrows)]
        return pltpu.make_async_remote_copy(src_ref=own, dst_ref=own, send_sem=hs_sem.at[c], recv_sem=hr_sem.at[c],
                                            device_id=sib, device_id_type=MESH)

    def chunk(c):
        x1_copy(c).wait()
        for n in range(nt):
            x_copy(0, c, n).wait_recv()

        def ln_rows(r, carry):
            rows = pl.ds(pl.multiple_of(r * 16, 16), 16)
            total = jnp.concatenate(
                [(ub[c * 2 + core, n, rows, :].astype(F32) + xrv[0, c, n, rows, :].astype(F32)).astype(BF) for n in range(nt)], axis=-1)
            mid = (x1[c, rows, :].astype(F32) + total.astype(F32)).astype(BF)
            x1[c, rows, :] = mid
            hrow = pl.ds(pl.multiple_of(core * hrows + r * 16, 16), 16)
            h2[c, hrow, :] = layer_norm(mid.astype(F32), g_ref[...], b_ref[...]).astype(BF)
            return carry
        lax.fori_loop(0, hrows // 16, ln_rows, 0)
        h_copy(c).start()

        def drain(n, carry):
            d_copy(0, c, n).wait_send()
            x_copy(0, c, n).wait_send()
            return carry
        lax.fori_loop(0, nt, drain, 0)
        h_copy(c).wait_recv()

        def up_step(n, carry):
            if c == 0:
                wup_copy(n).wait()
            res = dot(h2[c], wa[n])
            res = 0.5 * res * (1.0 + lax.erf(res * (0.5 ** 0.5)))
            zb[c * 2 * hrows:(c + 1) * 2 * hrows, pl.ds(pl.multiple_of(n * 256, 256), 256)] = res.astype(BF)
            return carry
        lax.fori_loop(0, ku, up_step, 0)

        def down_step(n, carry):
            if c == 0:
                wdn_copy(n).wait()
            res = dot(zb[c * 2 * hrows:(c + 1) * 2 * hrows, :], wbb[n]).astype(BF)
            for j in range(2):
                ub[c * 2 + j, n] = res[j * hrows:(j + 1) * hrows]
            d_copy(1, c, n).start()

            @pl.when(n >= lag)
            def _():
                forward(1, c, n - lag)
            return carry
        lax.fori_loop(0, nt, down_step, 0)
        for n in range(nt - lag, nt):
            forward(1, c, n)

    chunk(0)
    chunk(1)

    def o_copies(c, n):
        src = x1.at[c, :, pl.ds(pl.multiple_of(n * TN, TN), TN)]
        dst = o_hbm.at[pl.ds(pl.multiple_of((c * 2 + core) * hrows, hrows), hrows), pl.ds(pl.multiple_of(n * TN, TN), TN)]
        local = pltpu.make_async_copy(src, dst, ol_sem.at[c, n])
        remote = pltpu.make_async_remote_copy(src_ref=src, dst_ref=dst, send_sem=os_sem.at[c, n], recv_sem=or_sem.at[c, n],
                                              device_id=sib, device_id_type=MESH)
        return local, remote

    for c in range(2):
        def out_step(n, carry):
            x_copy(1, c, n).wait_recv()
            cols = pl.ds(pl.multiple_of(n * TN, TN), TN)
            total = (ub[c * 2 + core, n].astype(F32) + xrv[1, c, n].astype(F32)).astype(BF)
            x1[c, :, cols] = (x1[c, :, cols].astype(F32) + total.astype(F32)).astype(BF)
            local, remote = o_copies(c, n)
            remote.start()
            local.start()
            return carry
        lax.fori_loop(0, nt, out_step, 0)
    for c in range(2):
        h_copy(c).wait_send()

        def fin(n, carry):
            d_copy(1, c, n).wait_send()
            x_copy(1, c, n).wait_send()
            local, remote = o_copies(c, n)
            local.wait()
            remote.wait_send()
            remote.wait_recv()
            return carry
        lax.fori_loop(0, nt, fin, 0)


def ffn_call(z2d, x2d, gain, bias, w_o, w_up, w_down):
    rows, d_model = x2d.shape
    width = z2d.shape[1]
    fdim = w_up.shape[1]
    nt = d_model // TN
    ku = fdim // 256
    hr = rows // 4
    anyspec = pl.BlockSpec(memory_space=pl.ANY)
    vspec = pl.BlockSpec(memory_space=pltpu.VMEM)
    dma = pltpu.SemaphoreType.DMA
    return pl.pallas_call(
        ffn_kernel,
        out_shape=jax.ShapeDtypeStruct((rows, d_model), BF),
        in_specs=[anyspec, anyspec, vspec, vspec, anyspec, anyspec, anyspec],
        out_specs=anyspec,
        scratch_shapes=[
            pltpu.VMEM((rows, width), BF),
            pltpu.VMEM((ku, d_model, 256), BF),
            pltpu.VMEM((nt, width, TN), BF),
            pltpu.VMEM((4, nt, hr, TN), BF),
            pltpu.VMEM((2, nt, hr, TN), BF),
            pltpu.VMEM((2, 2, nt, hr, TN), BF),
            pltpu.VMEM((2, 2 * hr, d_model), BF),
            pltpu.VMEM((2, hr, d_model), BF),
            dma, dma((2,)), dma((nt,)), dma((ku,)), dma((nt,)),
            dma((2, 2, nt)), dma((2, 2, nt)), dma((2, 2, nt)), dma((2, 2, nt)), dma((2,)), dma((2,)),
            dma((2, nt)), dma((2, nt)), dma((2, nt)),
        ],
        compiler_params=pltpu.CompilerParams(collective_id=0, has_side_effects=True, vmem_limit_bytes=67043328),
        cost_estimate=pl.CostEstimate(flops=20_000_000_000, bytes_accessed=85_000_000, transcendentals=0),
        name='ffn',
    )(z2d, x2d, gain, bias, w_o, w_up, w_down)


def solution(mesh):
    def local_layer(x_in, start_pos, kv_state, ln1_gain, ln1_bias, w_q, w_k, w_v, w_g, w_o, ln2_gain, ln2_bias, w_up, w_down):
        nseq, clen, d_model = x_in.shape
        x2d = x_in.reshape(nseq * clen, d_model)
        cos_t, sin_t = rope_tables(start_pos, clen, kv_state.shape[2])
        num_heads = kv_state.shape[1] * mesh.shape['tp']
        log_gammas = jnp.asarray(np.log1p(-np.exp2(-5.0 - np.arange(num_heads))).astype(np.float32))
        z2d, new_state = mix_call(x2d, cos_t, sin_t, ln1_gain.reshape(1, -1), ln1_bias.reshape(1, -1),
                                  w_q, w_k, w_v, w_g, kv_state, log_gammas)
        out = ffn_call(z2d, x2d, ln2_gain.reshape(1, -1), ln2_bias.reshape(1, -1), w_o, w_up, w_down)
        return out.reshape(x_in.shape), new_state

    in_specs = (P('dp', None, None), P('dp'), P('dp', 'tp', None, None), P(), P(), P(None, 'tp'), P(None, 'tp'), P(None, 'tp'), P(None, 'tp'), P('tp', None), P(), P(), P(None, 'tp'), P('tp', None))
    out_specs = (P('dp', None, None), P('dp', 'tp', None, None))
    return jax.shard_map(local_layer, mesh=mesh, in_specs=in_specs, out_specs=out_specs, check_vma=False)
```

```python
import numpy as np
import jax
import jax.numpy as jnp
from jax import lax
from jax.experimental import pallas as pl
from jax.experimental.pallas import tpu as pltpu
from jax.sharding import PartitionSpec as P

NORM_EPS = 1e-5
GROUP_EPS = 1e-6
ROPE_BASE = 10000.0
BF = jnp.bfloat16
F32 = jnp.float32
MESH = pl.DeviceIdType.MESH
SLOTS = 4


def layer_norm(x_f32, norm_gain, norm_bias):
    row_mean = jnp.mean(x_f32, axis=-1, keepdims=True)
    centered = x_f32 - row_mean
    variance = jnp.mean(centered * centered, axis=-1, keepdims=True)
    return centered * lax.rsqrt(variance + NORM_EPS) * norm_gain + norm_bias


def rope_constants(chunk_len, key_dim):
    half_dim = key_dim // 2
    inv_freq = np.power(ROPE_BASE, -np.arange(half_dim) / half_dim).astype(np.float32)
    step_angles = np.arange(chunk_len)[:, None] * inv_freq.astype(np.float64)[None, :]
    return jnp.asarray(inv_freq[None, :]), jnp.asarray(np.cos(step_angles).astype(np.float32)), jnp.asarray(np.sin(step_angles).astype(np.float32))


def split2(val):
    high = val.astype(BF)
    return high, (val - high.astype(F32)).astype(BF)


def dot(lhs, rhs):
    return jnp.dot(lhs, rhs, preferred_element_type=F32)


def ln_rows(load, store, g_ref, b_ref, width):
    cols = [slice(c, c + 256) for c in range(0, width, 256)]
    total = load(cols[0])
    for col in cols[1:]:
        total = total + load(col)
    mean = jnp.sum(total, axis=-1, keepdims=True) * (1.0 / width)
    total = None
    for col in cols:
        cent = load(col) - mean
        total = cent * cent if total is None else total + cent * cent
    var = jnp.sum(total, axis=-1, keepdims=True) * (1.0 / width)
    scale = lax.rsqrt(var + NORM_EPS)
    for col in cols:
        store(col, ((load(col) - mean) * scale * g_ref[:, col] + b_ref[:, col]).astype(BF))


def mix_kernel(lg_ref, pos_ref, x_hbm, freq_ref, stepc_ref, steps_ref, g_ref, b_ref, wq, wk, wv, wg, s_hbm, z_hbm, so_hbm,
               cos_ref, sin_ref, xb, hb, wb, sb, sob, qb, kb, vb, gb, scb, sth, stl, kdb, ob, zb, xsem, wsem, ssem, sosem, zsem):
    heads = wq.shape[1] // 256
    nseq = s_hbm.shape[0]
    clen = x_hbm.shape[0] // nseq
    first_head = lax.axis_index('tp') * heads

    def wcopies(head, i):
        slot = lax.rem(head * 3 + i, SLOTS)
        wide = pl.ds(pl.multiple_of(head * 512, 512), 512)
        narrow = pl.ds(pl.multiple_of(head * 256, 256), 256)
        if i == 0:
            return (pltpu.make_async_copy(wq.at[:, narrow], wb.at[slot, :, :256], wsem.at[slot, 0]),
                    pltpu.make_async_copy(wk.at[:, narrow], wb.at[slot, :, 256:], wsem.at[slot, 1]))
        return (pltpu.make_async_copy((wv if i == 1 else wg).at[:, wide], wb.at[slot], wsem.at[slot, 0]),)

    def wstart(head, i):
        for copy in wcopies(head, i):
            copy.start()

    def scopy(head):
        slot = lax.rem(head, 2)
        return pltpu.make_async_copy(s_hbm.at[:, head], sb.at[slot], ssem.at[slot])

    def socopy(head):
        slot = lax.rem(head, 2)
        return pltpu.make_async_copy(sob.at[slot], so_hbm.at[:, head], sosem.at[slot])

    def zcopy(head):
        slot = lax.rem(head, 2)
        return pltpu.make_async_copy(zb.at[slot], z_hbm.at[:, pl.ds(pl.multiple_of(head * 512, 512), 512)], zsem.at[slot])

    def xcopy(s):
        rows = pl.ds(pl.multiple_of(s * clen, clen), clen)
        return pltpu.make_async_copy(x_hbm.at[rows], xb.at[rows], xsem.at[s])

    for s in range(nseq):
        xcopy(s).start()
    wstart(0, 0)

    def ln_body(s, carry):
        @pl.when(s < nseq - 1)
        def _():
            xcopy(s).wait()
        rows = pl.ds(pl.multiple_of(s * clen, clen), clen)

        def store(col, val):
            hb[rows, col] = val
        ln_rows(lambda col: xb[rows, col].astype(F32), store, g_ref, b_ref, xb.shape[1])
        return carry
    def rope_body(s, carry):
        angle = pos_ref[s].astype(F32) * freq_ref[...]
        base_c, base_s = jnp.cos(angle), jnp.sin(angle)
        rows = pl.ds(pl.multiple_of(s * clen, clen), clen)
        cos_ref[rows, :] = base_c * stepc_ref[...] - base_s * steps_ref[...]
        sin_ref[rows, :] = base_s * stepc_ref[...] + base_c * steps_ref[...]
        return carry
    lax.fori_loop(0, nseq, rope_body, 0)

    xcopy(nseq - 1).wait()
    for i in range(1, SLOTS):
        wstart(i // 3, i % 3)
    scopy(0).start()
    scopy(1).start()
    lax.fori_loop(0, nseq, ln_body, 0)

    step_i = lax.broadcasted_iota(jnp.int32, (clen, clen), 0)
    step_j = lax.broadcasted_iota(jnp.int32, (clen, clen), 1)
    gap = step_i - step_j
    tok_q = lax.broadcasted_iota(jnp.int32, (clen, 512), 0).astype(F32)
    tok_k = lax.broadcasted_iota(jnp.int32, (clen, 256), 0).astype(F32)

    def project(head, i):
        return dot(hb[...], wb[lax.rem(head * 3 + i, SLOTS)])

    def wwait(head, i):
        for copy in wcopies(head, i):
            copy.wait()

    def wnext(head, i):
        next_head, next_i = head + (i + SLOTS) // 3, (i + SLOTS) % 3

        @pl.when(next_head < heads)
        def _():
            wstart(next_head, next_i)

    def proj_qk(head, slot):
        cos_t = cos_ref[...]
        sin_t = sin_ref[...]
        qk = project(head, 0)
        q, k = qk[:, :256], qk[:, 256:]
        qb[slot, :, :128] = (q[:, :128] * cos_t - q[:, 128:] * sin_t).astype(BF)
        qb[slot, :, 128:] = (q[:, 128:] * cos_t + q[:, :128] * sin_t).astype(BF)
        kb[slot, :, :128] = ((k[:, :128] * cos_t - k[:, 128:] * sin_t) * 0.0625).astype(BF)
        kb[slot, :, 128:] = ((k[:, 128:] * cos_t + k[:, :128] * sin_t) * 0.0625).astype(BF)

    def proj_v(head, slot):
        val = project(head, 1).astype(BF)
        for s in range(nseq):
            for copy in range(2):
                vb[slot, s, copy * clen:(copy + 1) * clen, :] = val[s * clen:(s + 1) * clen]

    def proj_g(head, slot):
        gb[slot] = project(head, 2)

    def seq_rows(s):
        return slice(s * clen, (s + 1) * clen)

    def ret_scores(slot):
        return [lax.dot_general(qb[slot, seq_rows(s), :], kb[slot, seq_rows(s), :], (((1,), (1,)), ((), ())),
                                preferred_element_type=F32) for s in range(nseq)]

    def ret_prepare(head, slot, scores):
        log_g = lg_ref[first_head + head]
        inner_decay = jnp.where(gap >= 0, jnp.exp(jnp.maximum(gap, 0).astype(F32) * log_g), 0.0)
        key_decay = jnp.exp((clen - 1.0 - tok_k) * log_g)
        for s in range(nseq):
            sth[s], stl[s] = split2(sb[slot, s])
            kdb[s, :clen], kdb[s, clen:] = split2(kb[slot, seq_rows(s), :].astype(F32) * key_decay)
            high, low = split2(scores[s] * inner_decay)
            scb[s] = jnp.concatenate([high, low], axis=-1)

    def ret_out(head, slot):
        log_g = lg_ref[first_head + head]
        query_decay = jnp.exp((tok_q + 1.0) * log_g)
        state_decay = jnp.exp(jnp.full((1, 512), clen, F32) * log_g)
        for s in range(nseq):
            q = qb[slot, seq_rows(s), :]
            ob[seq_rows(s), :] = dot(scb[s], vb[slot, s]) + (dot(q, sth[s]) + dot(q, stl[s])) * query_decay
            update = lax.dot_general(kdb[s], vb[slot, s], (((0,), (0,)), ((), ())), preferred_element_type=F32)
            sob[slot, s] = sb[slot, s] * state_decay + update

    def ret_gate(slot):
        for s in range(nseq):
            out = ob[seq_rows(s), :]
            mean = jnp.mean(out, axis=-1, keepdims=True)
            cent = out - mean
            var = jnp.mean(cent * cent, axis=-1, keepdims=True)
            gates = gb[slot, seq_rows(s), :]
            zb[slot, seq_rows(s), :] = (gates * jax.nn.sigmoid(gates) * (cent * lax.rsqrt(var + GROUP_EPS))).astype(BF)

    wwait(0, 0)
    proj_qk(0, 0)
    wnext(0, 0)
    wwait(0, 1)
    proj_v(0, 0)
    wnext(0, 1)
    wwait(0, 2)
    proj_g(0, 0)
    wnext(0, 2)

    def head_body(head, carry):
        prev = head - 1
        slot = lax.rem(head, 2)
        old = 1 - slot
        scopy(prev).wait()

        @pl.when(prev >= 2)
        def _():
            socopy(prev - 2).wait()
            zcopy(prev - 2).wait()
        wwait(head, 0)
        scores = ret_scores(old)
        proj_qk(head, slot)
        ret_prepare(prev, old, scores)
        wnext(head, 0)
        wwait(head, 1)
        ret_out(prev, old)
        proj_v(head, slot)
        wnext(head, 1)
        socopy(prev).start()

        @pl.when(head + 1 < heads)
        def _():
            scopy(head + 1).start()
        wwait(head, 2)
        proj_g(head, slot)
        ret_gate(old)
        wnext(head, 2)
        zcopy(prev).start()
        return carry

    lax.fori_loop(1, heads, head_body, 0)
    last = heads - 1
    slot = last % 2
    scopy(last).wait()
    socopy(last - 2).wait()
    zcopy(last - 2).wait()
    ret_prepare(last, slot, ret_scores(slot))
    ret_out(last, slot)
    socopy(last).start()
    ret_gate(slot)
    zcopy(last).start()
    for head in (last - 1, last):
        socopy(head).wait()
        zcopy(head).wait()


def mix_call(x2d, start_pos, gain, bias, w_q, w_k, w_v, w_g, state, log_gammas):
    rows, d_model = x2d.shape
    nseq, heads = state.shape[:2]
    clen = rows // nseq
    smem = pl.BlockSpec(memory_space=pltpu.SMEM)
    anyspec = pl.BlockSpec(memory_space=pl.ANY)
    vspec = pl.BlockSpec(memory_space=pltpu.VMEM)
    return pl.pallas_call(
        mix_kernel,
        out_shape=(jax.ShapeDtypeStruct((rows, heads * 512), BF), jax.ShapeDtypeStruct(state.shape, F32)),
        in_specs=[smem, smem, anyspec] + [vspec] * 5 + [anyspec] * 5,
        out_specs=(anyspec, anyspec),
        scratch_shapes=[
            pltpu.VMEM((rows, 128), F32), pltpu.VMEM((rows, 128), F32),
            pltpu.VMEM((rows, d_model), BF), pltpu.VMEM((rows, d_model), BF),
            pltpu.VMEM((SLOTS, d_model, 512), BF),
            pltpu.VMEM((2, nseq, 256, 512), F32), pltpu.VMEM((2, nseq, 256, 512), F32),
            pltpu.VMEM((2, rows, 256), BF), pltpu.VMEM((2, rows, 256), BF), pltpu.VMEM((2, nseq, 2 * clen, 512), BF),
            pltpu.VMEM((2, rows, 512), F32),
            pltpu.VMEM((nseq, clen, 2 * clen), BF), pltpu.VMEM((nseq, 256, 512), BF), pltpu.VMEM((nseq, 256, 512), BF),
            pltpu.VMEM((nseq, 2 * clen, 256), BF), pltpu.VMEM((rows, 512), F32), pltpu.VMEM((2, rows, 512), BF),
            pltpu.SemaphoreType.DMA((nseq,)), pltpu.SemaphoreType.DMA((SLOTS, 2)), pltpu.SemaphoreType.DMA((2,)),
            pltpu.SemaphoreType.DMA((2,)), pltpu.SemaphoreType.DMA((2,)),
        ],
        compiler_params=pltpu.CompilerParams(vmem_limit_bytes=60 * 1024 * 1024),
        cost_estimate=pl.CostEstimate(flops=21_000_000_000, bytes_accessed=102_000_000, transcendentals=0),
        name='mix',
    )(log_gammas, start_pos, x2d, *rope_constants(clen, state.shape[2]), gain, bias, w_q, w_k, w_v, w_g, state)


TN = 512


def ffn_kernel(z_hbm, x_hbm, g_ref, b_ref, wo, wup, wdn, o_hbm,
               zb, wa, wbb, ub, drv, xrv, h2, x1,
               zsem, x1sem, wosem, wupsem, wdnsem, ds_sem, dr_sem, xs_sem, xr_sem, hs_sem, hr_sem, ol_sem, os_sem, or_sem):
    tp = lax.axis_index('tp')
    core = lax.rem(tp, 2)
    sib = {'tp': tp + 1 - 2 * core}
    nbr = {'tp': lax.rem(tp + 2, 4)}
    nt = wo.shape[1] // TN
    ku = wup.shape[1] // 256
    hrows = ub.shape[2]

    def wo_copy(n):
        return pltpu.make_async_copy(wo.at[:, pl.ds(pl.multiple_of(n * TN, TN), TN)], wbb.at[n], wosem.at[n])

    def wdn_copy(n):
        return pltpu.make_async_copy(wdn.at[:, pl.ds(pl.multiple_of(n * TN, TN), TN)], wbb.at[n], wdnsem.at[n])

    def wup_copy(n):
        return pltpu.make_async_copy(wup.at[:, pl.ds(pl.multiple_of(n * 256, 256), 256)], wa.at[n], wupsem.at[n])

    def x1_copy(c):
        src = x_hbm.at[pl.ds(pl.multiple_of((c * 2 + core) * hrows, hrows), hrows)]
        return pltpu.make_async_copy(src, x1.at[c], x1sem.at[c])

    zcopy = pltpu.make_async_copy(z_hbm, zb, zsem)
    zcopy.start()

    def start_wo(n, carry):
        wo_copy(n).start()
        return carry
    lax.fori_loop(0, nt, start_wo, 0)
    x1_copy(0).start(priority=1)
    x1_copy(1).start(priority=1)

    def start_wup(n, carry):
        wup_copy(n).start(priority=1)
        return carry
    lax.fori_loop(0, ku, start_wup, 0)

    barrier = pltpu.get_barrier_semaphore()
    pl.semaphore_signal(barrier, inc=1, device_id=sib, device_id_type=MESH)
    pl.semaphore_signal(barrier, inc=1, device_id=nbr, device_id_type=MESH)
    pl.semaphore_wait(barrier, 2)

    def d_copy(r, c, n):
        return pltpu.make_async_remote_copy(
            src_ref=ub.at[c * 2 + 1 - core, n], dst_ref=drv.at[c, n], send_sem=ds_sem.at[r, c, n], recv_sem=dr_sem.at[r, c, n],
            device_id=sib, device_id_type=MESH)

    def x_copy(r, c, n):
        return pltpu.make_async_remote_copy(
            src_ref=ub.at[c * 2 + core, n], dst_ref=xrv.at[r, c, n], send_sem=xs_sem.at[r, c, n], recv_sem=xr_sem.at[r, c, n],
            device_id=nbr, device_id_type=MESH)

    def forward(r, c, n):
        d_copy(r, c, n).wait_recv()
        own = ub[c * 2 + core, n].astype(F32)
        ub[c * 2 + core, n] = (own + drv[c, n].astype(F32)).astype(BF)
        x_copy(r, c, n).start()

    lag = 2
    zcopy.wait()

    def wo_step(n, carry):
        wo_copy(n).wait()
        res = dot(zb[...], wbb[n]).astype(BF)
        for j in range(4):
            ub[j, n] = res[j * hrows:(j + 1) * hrows]
        d_copy(0, 0, n).start()
        d_copy(0, 1, n).start()
        wdn_copy(n).start(priority=1)

        @pl.when(n >= 1)
        def _():
            forward(0, 0, n - 1)
        return carry
    lax.fori_loop(0, nt, wo_step, 0)
    forward(0, 0, nt - 1)

    def fwd1(n, carry):
        forward(0, 1, n)
        return carry
    lax.fori_loop(0, nt, fwd1, 0)

    def h_copy(c):
        own = h2.at[c, pl.ds(pl.multiple_of(core * hrows, hrows), hrows)]
        return pltpu.make_async_remote_copy(src_ref=own, dst_ref=own, send_sem=hs_sem.at[c], recv_sem=hr_sem.at[c],
                                            device_id=sib, device_id_type=MESH)

    def chunk(c):
        x1_copy(c).wait()
        for n in range(nt):
            x_copy(0, c, n).wait_recv()

        def ln_rows(r, carry):
            rows = pl.ds(pl.multiple_of(r * 16, 16), 16)
            total = jnp.concatenate(
                [(ub[c * 2 + core, n, rows, :].astype(F32) + xrv[0, c, n, rows, :].astype(F32)).astype(BF) for n in range(nt)], axis=-1)
            mid = (x1[c, rows, :].astype(F32) + total.astype(F32)).astype(BF)
            x1[c, rows, :] = mid
            hrow = pl.ds(pl.multiple_of(core * hrows + r * 16, 16), 16)
            h2[c, hrow, :] = layer_norm(mid.astype(F32), g_ref[...], b_ref[...]).astype(BF)
            return carry
        lax.fori_loop(0, hrows // 16, ln_rows, 0)
        h_copy(c).start()

        def drain(n, carry):
            d_copy(0, c, n).wait_send()
            x_copy(0, c, n).wait_send()
            return carry
        lax.fori_loop(0, nt, drain, 0)
        h_copy(c).wait_recv()

        def up_step(n, carry):
            if c == 0:
                wup_copy(n).wait()
            res = dot(h2[c], wa[n])
            res = 0.5 * res * (1.0 + lax.erf(res * (0.5 ** 0.5)))
            zb[c * 2 * hrows:(c + 1) * 2 * hrows, pl.ds(pl.multiple_of(n * 256, 256), 256)] = res.astype(BF)
            return carry
        lax.fori_loop(0, ku, up_step, 0)

        def down_step(n, carry):
            if c == 0:
                wdn_copy(n).wait()
            res = dot(zb[c * 2 * hrows:(c + 1) * 2 * hrows, :], wbb[n]).astype(BF)
            for j in range(2):
                ub[c * 2 + j, n] = res[j * hrows:(j + 1) * hrows]
            d_copy(1, c, n).start()

            @pl.when(n >= lag)
            def _():
                forward(1, c, n - lag)
            return carry
        lax.fori_loop(0, nt, down_step, 0)
        for n in range(nt - lag, nt):
            forward(1, c, n)

    chunk(0)
    chunk(1)

    def o_copies(c, n):
        src = x1.at[c, :, pl.ds(pl.multiple_of(n * TN, TN), TN)]
        dst = o_hbm.at[pl.ds(pl.multiple_of((c * 2 + core) * hrows, hrows), hrows), pl.ds(pl.multiple_of(n * TN, TN), TN)]
        local = pltpu.make_async_copy(src, dst, ol_sem.at[c, n])
        remote = pltpu.make_async_remote_copy(src_ref=src, dst_ref=dst, send_sem=os_sem.at[c, n], recv_sem=or_sem.at[c, n],
                                              device_id=sib, device_id_type=MESH)
        return local, remote

    for c in range(2):
        def out_step(n, carry):
            x_copy(1, c, n).wait_recv()
            cols = pl.ds(pl.multiple_of(n * TN, TN), TN)
            total = (ub[c * 2 + core, n].astype(F32) + xrv[1, c, n].astype(F32)).astype(BF)
            x1[c, :, cols] = (x1[c, :, cols].astype(F32) + total.astype(F32)).astype(BF)
            local, remote = o_copies(c, n)
            remote.start()
            local.start()
            return carry
        lax.fori_loop(0, nt, out_step, 0)
    for c in range(2):
        h_copy(c).wait_send()

        def fin(n, carry):
            d_copy(1, c, n).wait_send()
            x_copy(1, c, n).wait_send()
            local, remote = o_copies(c, n)
            local.wait()
            remote.wait_send()
            remote.wait_recv()
            return carry
        lax.fori_loop(0, nt, fin, 0)


def ffn_call(z2d, x2d, gain, bias, w_o, w_up, w_down):
    rows, d_model = x2d.shape
    width = z2d.shape[1]
    fdim = w_up.shape[1]
    nt = d_model // TN
    ku = fdim // 256
    hr = rows // 4
    anyspec = pl.BlockSpec(memory_space=pl.ANY)
    vspec = pl.BlockSpec(memory_space=pltpu.VMEM)
    dma = pltpu.SemaphoreType.DMA
    return pl.pallas_call(
        ffn_kernel,
        out_shape=jax.ShapeDtypeStruct((rows, d_model), BF),
        in_specs=[anyspec, anyspec, vspec, vspec, anyspec, anyspec, anyspec],
        out_specs=anyspec,
        scratch_shapes=[
            pltpu.VMEM((rows, width), BF),
            pltpu.VMEM((ku, d_model, 256), BF),
            pltpu.VMEM((nt, width, TN), BF),
            pltpu.VMEM((4, nt, hr, TN), BF),
            pltpu.VMEM((2, nt, hr, TN), BF),
            pltpu.VMEM((2, 2, nt, hr, TN), BF),
            pltpu.VMEM((2, 2 * hr, d_model), BF),
            pltpu.VMEM((2, hr, d_model), BF),
            dma, dma((2,)), dma((nt,)), dma((ku,)), dma((nt,)),
            dma((2, 2, nt)), dma((2, 2, nt)), dma((2, 2, nt)), dma((2, 2, nt)), dma((2,)), dma((2,)),
            dma((2, nt)), dma((2, nt)), dma((2, nt)),
        ],
        compiler_params=pltpu.CompilerParams(collective_id=0, has_side_effects=True, vmem_limit_bytes=67043328),
        cost_estimate=pl.CostEstimate(flops=20_000_000_000, bytes_accessed=85_000_000, transcendentals=0),
        name='ffn',
    )(z2d, x2d, gain, bias, w_o, w_up, w_down)


def solution(mesh):
    def local_layer(x_in, start_pos, kv_state, ln1_gain, ln1_bias, w_q, w_k, w_v, w_g, w_o, ln2_gain, ln2_bias, w_up, w_down):
        nseq, clen, d_model = x_in.shape
        x2d = x_in.reshape(nseq * clen, d_model)
        num_heads = kv_state.shape[1] * mesh.shape['tp']
        log_gammas = jnp.asarray(np.log1p(-np.exp2(-5.0 - np.arange(num_heads))).astype(np.float32))
        z2d, new_state = mix_call(x2d, start_pos, ln1_gain.reshape(1, -1), ln1_bias.reshape(1, -1),
                                  w_q, w_k, w_v, w_g, kv_state, log_gammas)
        out = ffn_call(z2d, x2d, ln2_gain.reshape(1, -1), ln2_bias.reshape(1, -1), w_o, w_up, w_down)
        return out.reshape(x_in.shape), new_state

    in_specs = (P('dp', None, None), P('dp'), P('dp', 'tp', None, None), P(), P(), P(None, 'tp'), P(None, 'tp'), P(None, 'tp'), P(None, 'tp'), P('tp', None), P(), P(), P(None, 'tp'), P('tp', None))
    out_specs = (P('dp', None, None), P('dp', 'tp', None, None))
    return jax.shard_map(local_layer, mesh=mesh, in_specs=in_specs, out_specs=out_specs, check_vma=False)
```

```python
import numpy as np
import jax
import jax.numpy as jnp
from jax import lax
from jax.experimental import pallas as pl
from jax.experimental.pallas import tpu as pltpu
from jax.sharding import PartitionSpec as P

NORM_EPS = 1e-5
GROUP_EPS = 1e-6
ROPE_BASE = 10000.0
BF = jnp.bfloat16
F32 = jnp.float32
MESH = pl.DeviceIdType.MESH
SLOTS = 4


def layer_norm(x_f32, norm_gain, norm_bias):
    row_mean = jnp.mean(x_f32, axis=-1, keepdims=True)
    centered = x_f32 - row_mean
    variance = jnp.mean(centered * centered, axis=-1, keepdims=True)
    return centered * lax.rsqrt(variance + NORM_EPS) * norm_gain + norm_bias


def rope_constants(chunk_len, key_dim):
    half_dim = key_dim // 2
    inv_freq = np.power(ROPE_BASE, -np.arange(half_dim) / half_dim).astype(np.float32)
    step_angles = np.arange(chunk_len)[:, None] * inv_freq.astype(np.float64)[None, :]
    return jnp.asarray(inv_freq[None, :]), jnp.asarray(np.cos(step_angles).astype(np.float32)), jnp.asarray(np.sin(step_angles).astype(np.float32))


def split2(val):
    high = val.astype(BF)
    return high, (val - high.astype(F32)).astype(BF)


def dot(lhs, rhs):
    return jnp.dot(lhs, rhs, preferred_element_type=F32)


def ln_rows(load, store, g_ref, b_ref, width):
    cols = [slice(c, c + 256) for c in range(0, width, 256)]
    total = load(cols[0])
    for col in cols[1:]:
        total = total + load(col)
    mean = jnp.sum(total, axis=-1, keepdims=True) * (1.0 / width)
    total = None
    for col in cols:
        cent = load(col) - mean
        total = cent * cent if total is None else total + cent * cent
    var = jnp.sum(total, axis=-1, keepdims=True) * (1.0 / width)
    scale = lax.rsqrt(var + NORM_EPS)
    for col in cols:
        store(col, ((load(col) - mean) * scale * g_ref[:, col] + b_ref[:, col]).astype(BF))


def mix_kernel(lg_hbm, pos_hbm, x_hbm, freq_hbm, stepc_hbm, steps_hbm, g_hbm, b_hbm, wq, wk, wv, wg, s_hbm, z_hbm, so_hbm,
               lg_ref, pos_ref, freq_ref, stepc_ref, steps_ref, g_ref, b_ref, small_sem, cos_ref, sin_ref, xb, hb, wb, sb, sob, qb, kb, vb, gb, scb, sth, stl, kdb, ob, zb, xsem, wsem, ssem, sosem, zsem):
    heads = wq.shape[1] // 256
    nseq = s_hbm.shape[0]
    clen = x_hbm.shape[0] // nseq
    first_head = lax.axis_index('tp') * heads

    def wcopies(head, i):
        slot = lax.rem(head * 3 + i, SLOTS)
        wide = pl.ds(pl.multiple_of(head * 512, 512), 512)
        narrow = pl.ds(pl.multiple_of(head * 256, 256), 256)
        if i == 0:
            return (pltpu.make_async_copy(wq.at[:, narrow], wb.at[slot, :, :256], wsem.at[slot, 0]),
                    pltpu.make_async_copy(wk.at[:, narrow], wb.at[slot, :, 256:], wsem.at[slot, 1]))
        return (pltpu.make_async_copy((wv if i == 1 else wg).at[:, wide], wb.at[slot], wsem.at[slot, 0]),)

    def wstart(head, i):
        for copy in wcopies(head, i):
            copy.start()

    def scopy(head):
        slot = lax.rem(head, 2)
        return pltpu.make_async_copy(s_hbm.at[:, head], sb.at[slot], ssem.at[slot])

    def socopy(head):
        slot = lax.rem(head, 2)
        return pltpu.make_async_copy(sob.at[slot], so_hbm.at[:, head], sosem.at[slot])

    def zcopy(head):
        slot = lax.rem(head, 2)
        return pltpu.make_async_copy(zb.at[slot], z_hbm.at[:, pl.ds(pl.multiple_of(head * 512, 512), 512)], zsem.at[slot])

    def xcopy(s):
        rows = pl.ds(pl.multiple_of(s * clen, clen), clen)
        return pltpu.make_async_copy(x_hbm.at[rows], xb.at[rows], xsem.at[s])

    small = ((pos_hbm, pos_ref), (freq_hbm, freq_ref), (stepc_hbm, stepc_ref), (steps_hbm, steps_ref),
             (g_hbm, g_ref), (b_hbm, b_ref), (lg_hbm, lg_ref))
    small = [pltpu.make_async_copy(src, dst, small_sem.at[i]) for i, (src, dst) in enumerate(small)]
    for copy in small:
        copy.start()
    for s in range(nseq):
        xcopy(s).start()
    wstart(0, 0)
    for copy in small:
        copy.wait()

    def ln_body(s, carry):
        xcopy(s).wait()

        @pl.when(s == nseq - 1)
        def _():
            for i in range(1, SLOTS):
                wstart(i // 3, i % 3)
            scopy(0).start()
            scopy(1).start()
        rows = pl.ds(pl.multiple_of(s * clen, clen), clen)

        def store(col, val):
            hb[rows, col] = val
        ln_rows(lambda col: xb[rows, col].astype(F32), store, g_ref, b_ref, xb.shape[1])
        return carry
    def rope_body(s, carry):
        angle = pos_ref[s].astype(F32) * freq_ref[...]
        base_c, base_s = jnp.cos(angle), jnp.sin(angle)
        rows = pl.ds(pl.multiple_of(s * clen, clen), clen)
        cos_ref[rows, :] = base_c * stepc_ref[...] - base_s * steps_ref[...]
        sin_ref[rows, :] = base_s * stepc_ref[...] + base_c * steps_ref[...]
        return carry
    lax.fori_loop(0, nseq, rope_body, 0)

    lax.fori_loop(0, nseq, ln_body, 0)

    step_i = lax.broadcasted_iota(jnp.int32, (clen, clen), 0)
    step_j = lax.broadcasted_iota(jnp.int32, (clen, clen), 1)
    gap = step_i - step_j
    tok_q = lax.broadcasted_iota(jnp.int32, (clen, 512), 0).astype(F32)
    tok_k = lax.broadcasted_iota(jnp.int32, (clen, 256), 0).astype(F32)

    def project(head, i):
        return dot(hb[...], wb[lax.rem(head * 3 + i, SLOTS)])

    def wwait(head, i):
        for copy in wcopies(head, i):
            copy.wait()

    def wnext(head, i):
        next_head, next_i = head + (i + SLOTS) // 3, (i + SLOTS) % 3

        @pl.when(next_head < heads)
        def _():
            wstart(next_head, next_i)

    def proj_qk(head, slot):
        cos_t = cos_ref[...]
        sin_t = sin_ref[...]
        qk = project(head, 0)
        q, k = qk[:, :256], qk[:, 256:]
        qb[slot, :, :128] = (q[:, :128] * cos_t - q[:, 128:] * sin_t).astype(BF)
        qb[slot, :, 128:] = (q[:, 128:] * cos_t + q[:, :128] * sin_t).astype(BF)
        kb[slot, :, :128] = ((k[:, :128] * cos_t - k[:, 128:] * sin_t) * 0.0625).astype(BF)
        kb[slot, :, 128:] = ((k[:, 128:] * cos_t + k[:, :128] * sin_t) * 0.0625).astype(BF)

    def proj_v(head, slot):
        val = project(head, 1).astype(BF)
        for s in range(nseq):
            for copy in range(2):
                vb[slot, s, copy * clen:(copy + 1) * clen, :] = val[s * clen:(s + 1) * clen]

    def proj_g(head, slot):
        gb[slot] = project(head, 2)

    def seq_rows(s):
        return slice(s * clen, (s + 1) * clen)

    def ret_scores(slot):
        return [lax.dot_general(qb[slot, seq_rows(s), :], kb[slot, seq_rows(s), :], (((1,), (1,)), ((), ())),
                                preferred_element_type=F32) for s in range(nseq)]

    def ret_prepare(head, slot, scores):
        log_g = lg_ref[first_head + head]
        inner_decay = jnp.where(gap >= 0, jnp.exp(jnp.maximum(gap, 0).astype(F32) * log_g), 0.0)
        key_decay = jnp.exp((clen - 1.0 - tok_k) * log_g)
        for s in range(nseq):
            sth[s], stl[s] = split2(sb[slot, s])
            kdb[s, :clen], kdb[s, clen:] = split2(kb[slot, seq_rows(s), :].astype(F32) * key_decay)
            high, low = split2(scores[s] * inner_decay)
            scb[s] = jnp.concatenate([high, low], axis=-1)

    def ret_out(head, slot):
        log_g = lg_ref[first_head + head]
        query_decay = jnp.exp((tok_q + 1.0) * log_g)
        state_decay = jnp.exp(jnp.full((1, 512), clen, F32) * log_g)
        for s in range(nseq):
            q = qb[slot, seq_rows(s), :]
            ob[seq_rows(s), :] = dot(scb[s], vb[slot, s]) + (dot(q, sth[s]) + dot(q, stl[s])) * query_decay
            update = lax.dot_general(kdb[s], vb[slot, s], (((0,), (0,)), ((), ())), preferred_element_type=F32)
            sob[slot, s] = sb[slot, s] * state_decay + update

    def ret_gate(slot):
        for s in range(nseq):
            out = ob[seq_rows(s), :]
            mean = jnp.mean(out, axis=-1, keepdims=True)
            cent = out - mean
            var = jnp.mean(cent * cent, axis=-1, keepdims=True)
            gates = gb[slot, seq_rows(s), :]
            zb[slot, seq_rows(s), :] = (gates * jax.nn.sigmoid(gates) * (cent * lax.rsqrt(var + GROUP_EPS))).astype(BF)

    wwait(0, 0)
    proj_qk(0, 0)
    wnext(0, 0)
    wwait(0, 1)
    proj_v(0, 0)
    wnext(0, 1)
    wwait(0, 2)
    proj_g(0, 0)
    wnext(0, 2)

    def head_body(head, carry):
        prev = head - 1
        slot = lax.rem(head, 2)
        old = 1 - slot
        scopy(prev).wait()

        @pl.when(prev >= 2)
        def _():
            socopy(prev - 2).wait()
            zcopy(prev - 2).wait()
        wwait(head, 0)
        scores = ret_scores(old)
        proj_qk(head, slot)
        ret_prepare(prev, old, scores)
        wnext(head, 0)
        wwait(head, 1)
        ret_out(prev, old)
        proj_v(head, slot)
        wnext(head, 1)
        socopy(prev).start()

        @pl.when(head + 1 < heads)
        def _():
            scopy(head + 1).start()
        wwait(head, 2)
        proj_g(head, slot)
        ret_gate(old)
        wnext(head, 2)
        zcopy(prev).start()
        return carry

    lax.fori_loop(1, heads, head_body, 0)
    last = heads - 1
    slot = last % 2
    scopy(last).wait()
    socopy(last - 2).wait()
    zcopy(last - 2).wait()
    ret_prepare(last, slot, ret_scores(slot))
    ret_out(last, slot)
    socopy(last).start()
    ret_gate(slot)
    zcopy(last).start()
    for head in (last - 1, last):
        socopy(head).wait()
        zcopy(head).wait()


def mix_call(x2d, start_pos, gain, bias, w_q, w_k, w_v, w_g, state, log_gammas):
    rows, d_model = x2d.shape
    nseq, heads = state.shape[:2]
    clen = rows // nseq
    anyspec = pl.BlockSpec(memory_space=pl.ANY)
    return pl.pallas_call(
        mix_kernel,
        out_shape=(jax.ShapeDtypeStruct((rows, heads * 512), BF), jax.ShapeDtypeStruct(state.shape, F32)),
        in_specs=[anyspec] * 13,
        out_specs=(anyspec, anyspec),
        scratch_shapes=[
            pltpu.SMEM(log_gammas.shape, F32), pltpu.SMEM(start_pos.shape, jnp.int32),
            pltpu.VMEM((1, 128), F32), pltpu.VMEM((clen, 128), F32), pltpu.VMEM((clen, 128), F32),
            pltpu.VMEM((1, d_model), F32), pltpu.VMEM((1, d_model), F32), pltpu.SemaphoreType.DMA((7,)),
            pltpu.VMEM((rows, 128), F32), pltpu.VMEM((rows, 128), F32),
            pltpu.VMEM((rows, d_model), BF), pltpu.VMEM((rows, d_model), BF),
            pltpu.VMEM((SLOTS, d_model, 512), BF),
            pltpu.VMEM((2, nseq, 256, 512), F32), pltpu.VMEM((2, nseq, 256, 512), F32),
            pltpu.VMEM((2, rows, 256), BF), pltpu.VMEM((2, rows, 256), BF), pltpu.VMEM((2, nseq, 2 * clen, 512), BF),
            pltpu.VMEM((2, rows, 512), F32),
            pltpu.VMEM((nseq, clen, 2 * clen), BF), pltpu.VMEM((nseq, 256, 512), BF), pltpu.VMEM((nseq, 256, 512), BF),
            pltpu.VMEM((nseq, 2 * clen, 256), BF), pltpu.VMEM((rows, 512), F32), pltpu.VMEM((2, rows, 512), BF),
            pltpu.SemaphoreType.DMA((nseq,)), pltpu.SemaphoreType.DMA((SLOTS, 2)), pltpu.SemaphoreType.DMA((2,)),
            pltpu.SemaphoreType.DMA((2,)), pltpu.SemaphoreType.DMA((2,)),
        ],
        compiler_params=pltpu.CompilerParams(vmem_limit_bytes=60 * 1024 * 1024),
        cost_estimate=pl.CostEstimate(flops=21_000_000_000, bytes_accessed=102_000_000, transcendentals=0),
        name='mix',
    )(log_gammas, start_pos, x2d, *rope_constants(clen, state.shape[2]), gain, bias, w_q, w_k, w_v, w_g, state)


TN = 512


def ffn_kernel(z_hbm, x_hbm, g_hbm, b_hbm, wo, wup, wdn, o_hbm,
               g_ref, b_ref, gb_sem, zb, wa, wbb, ub, drv, xrv, h2, x1,
               zsem, x1sem, wosem, wupsem, wdnsem, ds_sem, dr_sem, xs_sem, xr_sem, hs_sem, hr_sem, ol_sem, os_sem, or_sem):
    tp = lax.axis_index('tp')
    core = lax.rem(tp, 2)
    sib = {'tp': tp + 1 - 2 * core}
    nbr = {'tp': lax.rem(tp + 2, 4)}
    nt = wo.shape[1] // TN
    ku = wup.shape[1] // 256
    hrows = ub.shape[2]

    def wo_copy(n):
        return pltpu.make_async_copy(wo.at[:, pl.ds(pl.multiple_of(n * TN, TN), TN)], wbb.at[n], wosem.at[n])

    def wdn_copy(n):
        return pltpu.make_async_copy(wdn.at[:, pl.ds(pl.multiple_of(n * TN, TN), TN)], wbb.at[n], wdnsem.at[n])

    def wup_copy(n):
        return pltpu.make_async_copy(wup.at[:, pl.ds(pl.multiple_of(n * 256, 256), 256)], wa.at[n], wupsem.at[n])

    def x1_copy(c):
        src = x_hbm.at[pl.ds(pl.multiple_of((c * 2 + core) * hrows, hrows), hrows)]
        return pltpu.make_async_copy(src, x1.at[c], x1sem.at[c])

    zcopy = pltpu.make_async_copy(z_hbm, zb, zsem)
    zcopy.start()

    def start_wo(n, carry):
        wo_copy(n).start()
        return carry
    lax.fori_loop(0, nt, start_wo, 0)
    gain_copies = (pltpu.make_async_copy(g_hbm, g_ref, gb_sem.at[0]), pltpu.make_async_copy(b_hbm, b_ref, gb_sem.at[1]))
    for copy in gain_copies:
        copy.start(priority=1)
    x1_copy(0).start(priority=1)
    x1_copy(1).start(priority=1)

    def start_wup(n, carry):
        wup_copy(n).start(priority=1)
        return carry
    lax.fori_loop(0, ku, start_wup, 0)

    barrier = pltpu.get_barrier_semaphore()
    pl.semaphore_signal(barrier, inc=1, device_id=sib, device_id_type=MESH)
    pl.semaphore_signal(barrier, inc=1, device_id=nbr, device_id_type=MESH)
    pl.semaphore_wait(barrier, 2)

    def d_copy(r, c, n):
        return pltpu.make_async_remote_copy(
            src_ref=ub.at[c * 2 + 1 - core, n], dst_ref=drv.at[c, n], send_sem=ds_sem.at[r, c, n], recv_sem=dr_sem.at[r, c, n],
            device_id=sib, device_id_type=MESH)

    def x_copy(r, c, n):
        return pltpu.make_async_remote_copy(
            src_ref=ub.at[c * 2 + core, n], dst_ref=xrv.at[r, c, n], send_sem=xs_sem.at[r, c, n], recv_sem=xr_sem.at[r, c, n],
            device_id=nbr, device_id_type=MESH)

    def forward(r, c, n):
        d_copy(r, c, n).wait_recv()
        own = ub[c * 2 + core, n].astype(F32)
        ub[c * 2 + core, n] = (own + drv[c, n].astype(F32)).astype(BF)
        x_copy(r, c, n).start()

    lag = 2
    zcopy.wait()

    def wo_step(n, carry):
        wo_copy(n).wait()
        res = dot(zb[...], wbb[n]).astype(BF)
        for j in range(4):
            ub[j, n] = res[j * hrows:(j + 1) * hrows]
        d_copy(0, 0, n).start()
        d_copy(0, 1, n).start()
        wdn_copy(n).start(priority=1)

        @pl.when(n >= 1)
        def _():
            forward(0, 0, n - 1)
        return carry
    lax.fori_loop(0, nt, wo_step, 0)
    forward(0, 0, nt - 1)

    def fwd1(n, carry):
        forward(0, 1, n)
        return carry
    lax.fori_loop(0, nt, fwd1, 0)

    def h_copy(c):
        own = h2.at[c, pl.ds(pl.multiple_of(core * hrows, hrows), hrows)]
        return pltpu.make_async_remote_copy(src_ref=own, dst_ref=own, send_sem=hs_sem.at[c], recv_sem=hr_sem.at[c],
                                            device_id=sib, device_id_type=MESH)

    def chunk(c):
        x1_copy(c).wait()
        for n in range(nt):
            x_copy(0, c, n).wait_recv()

        def ln_rows(r, carry):
            rows = pl.ds(pl.multiple_of(r * 16, 16), 16)
            total = jnp.concatenate(
                [(ub[c * 2 + core, n, rows, :].astype(F32) + xrv[0, c, n, rows, :].astype(F32)).astype(BF) for n in range(nt)], axis=-1)
            mid = (x1[c, rows, :].astype(F32) + total.astype(F32)).astype(BF)
            x1[c, rows, :] = mid
            hrow = pl.ds(pl.multiple_of(core * hrows + r * 16, 16), 16)
            h2[c, hrow, :] = layer_norm(mid.astype(F32), g_ref[...], b_ref[...]).astype(BF)
            return carry
        lax.fori_loop(0, hrows // 16, ln_rows, 0)
        h_copy(c).start()

        def drain(n, carry):
            d_copy(0, c, n).wait_send()
            x_copy(0, c, n).wait_send()
            return carry
        lax.fori_loop(0, nt, drain, 0)
        h_copy(c).wait_recv()

        def up_step(n, carry):
            if c == 0:
                wup_copy(n).wait()
            res = dot(h2[c], wa[n])
            res = 0.5 * res * (1.0 + lax.erf(res * (0.5 ** 0.5)))
            zb[c * 2 * hrows:(c + 1) * 2 * hrows, pl.ds(pl.multiple_of(n * 256, 256), 256)] = res.astype(BF)
            return carry
        lax.fori_loop(0, ku, up_step, 0)

        def down_step(n, carry):
            if c == 0:
                wdn_copy(n).wait()
            res = dot(zb[c * 2 * hrows:(c + 1) * 2 * hrows, :], wbb[n]).astype(BF)
            for j in range(2):
                ub[c * 2 + j, n] = res[j * hrows:(j + 1) * hrows]
            d_copy(1, c, n).start()

            @pl.when(n >= lag)
            def _():
                forward(1, c, n - lag)
            return carry
        lax.fori_loop(0, nt, down_step, 0)
        for n in range(nt - lag, nt):
            forward(1, c, n)

    for copy in gain_copies:
        copy.wait()
    chunk(0)
    chunk(1)

    def o_copies(c, n):
        src = x1.at[c, :, pl.ds(pl.multiple_of(n * TN, TN), TN)]
        dst = o_hbm.at[pl.ds(pl.multiple_of((c * 2 + core) * hrows, hrows), hrows), pl.ds(pl.multiple_of(n * TN, TN), TN)]
        local = pltpu.make_async_copy(src, dst, ol_sem.at[c, n])
        remote = pltpu.make_async_remote_copy(src_ref=src, dst_ref=dst, send_sem=os_sem.at[c, n], recv_sem=or_sem.at[c, n],
                                              device_id=sib, device_id_type=MESH)
        return local, remote

    for c in range(2):
        def out_step(n, carry):
            x_copy(1, c, n).wait_recv()
            cols = pl.ds(pl.multiple_of(n * TN, TN), TN)
            total = (ub[c * 2 + core, n].astype(F32) + xrv[1, c, n].astype(F32)).astype(BF)
            x1[c, :, cols] = (x1[c, :, cols].astype(F32) + total.astype(F32)).astype(BF)
            local, remote = o_copies(c, n)
            remote.start()
            local.start()
            return carry
        lax.fori_loop(0, nt, out_step, 0)
    for c in range(2):
        h_copy(c).wait_send()

        def fin(n, carry):
            d_copy(1, c, n).wait_send()
            x_copy(1, c, n).wait_send()
            local, remote = o_copies(c, n)
            local.wait()
            remote.wait_send()
            remote.wait_recv()
            return carry
        lax.fori_loop(0, nt, fin, 0)


def ffn_call(z2d, x2d, gain, bias, w_o, w_up, w_down):
    rows, d_model = x2d.shape
    width = z2d.shape[1]
    fdim = w_up.shape[1]
    nt = d_model // TN
    ku = fdim // 256
    hr = rows // 4
    anyspec = pl.BlockSpec(memory_space=pl.ANY)
    dma = pltpu.SemaphoreType.DMA
    return pl.pallas_call(
        ffn_kernel,
        out_shape=jax.ShapeDtypeStruct((rows, d_model), BF),
        in_specs=[anyspec] * 7,
        out_specs=anyspec,
        scratch_shapes=[
            pltpu.VMEM((1, d_model), F32), pltpu.VMEM((1, d_model), F32), dma((2,)),
            pltpu.VMEM((rows, width), BF),
            pltpu.VMEM((ku, d_model, 256), BF),
            pltpu.VMEM((nt, width, TN), BF),
            pltpu.VMEM((4, nt, hr, TN), BF),
            pltpu.VMEM((2, nt, hr, TN), BF),
            pltpu.VMEM((2, 2, nt, hr, TN), BF),
            pltpu.VMEM((2, 2 * hr, d_model), BF),
            pltpu.VMEM((2, hr, d_model), BF),
            dma, dma((2,)), dma((nt,)), dma((ku,)), dma((nt,)),
            dma((2, 2, nt)), dma((2, 2, nt)), dma((2, 2, nt)), dma((2, 2, nt)), dma((2,)), dma((2,)),
            dma((2, nt)), dma((2, nt)), dma((2, nt)),
        ],
        compiler_params=pltpu.CompilerParams(collective_id=0, has_side_effects=True, vmem_limit_bytes=67043328),
        cost_estimate=pl.CostEstimate(flops=20_000_000_000, bytes_accessed=85_000_000, transcendentals=0),
        name='ffn',
    )(z2d, x2d, gain, bias, w_o, w_up, w_down)


def emit_kernel(src, dst, buf, in_sem, out_sem):
    parts = buf.shape[0]
    ins = [pltpu.make_async_copy(src.at[i], buf.at[i], in_sem.at[i]) for i in range(parts)]
    outs = [pltpu.make_async_copy(buf.at[i], dst.at[i], out_sem.at[i]) for i in range(parts)]
    for copy in ins:
        copy.start()
    for copy_in, copy_out in zip(ins, outs):
        copy_in.wait()
        copy_out.start()
    for copy in outs:
        copy.wait()


def emit_call(out):
    dma = pltpu.SemaphoreType.DMA
    anyspec = pl.BlockSpec(memory_space=pl.ANY)
    return pl.pallas_call(
        emit_kernel, out_shape=jax.ShapeDtypeStruct(out.shape, out.dtype), in_specs=[anyspec], out_specs=anyspec,
        scratch_shapes=[pltpu.VMEM(out.shape, out.dtype), dma((out.shape[0],)), dma((out.shape[0],))],
        compiler_params=pltpu.CompilerParams(vmem_limit_bytes=60 * 1024 * 1024),
        name='emit',
    )(out)


def solution(mesh):
    def local_layer(x_in, start_pos, kv_state, ln1_gain, ln1_bias, w_q, w_k, w_v, w_g, w_o, ln2_gain, ln2_bias, w_up, w_down):
        nseq, clen, d_model = x_in.shape
        x2d = x_in.reshape(nseq * clen, d_model)
        num_heads = kv_state.shape[1] * mesh.shape['tp']
        log_gammas = jnp.asarray(np.log1p(-np.exp2(-5.0 - np.arange(num_heads))).astype(np.float32))
        z2d, new_state = mix_call(x2d, start_pos, ln1_gain.reshape(1, -1), ln1_bias.reshape(1, -1),
                                  w_q, w_k, w_v, w_g, kv_state, log_gammas)
        out = ffn_call(z2d, x2d, ln2_gain.reshape(1, -1), ln2_bias.reshape(1, -1), w_o, w_up, w_down)
        return emit_call(out.reshape(16, -1, d_model)).reshape(x_in.shape), new_state

    in_specs = (P('dp', None, None), P('dp'), P('dp', 'tp', None, None), P(), P(), P(None, 'tp'), P(None, 'tp'), P(None, 'tp'), P(None, 'tp'), P('tp', None), P(), P(), P(None, 'tp'), P('tp', None))
    out_specs = (P('dp', None, None), P('dp', 'tp', None, None))
    return jax.shard_map(local_layer, mesh=mesh, in_specs=in_specs, out_specs=out_specs, check_vma=False)
```

```python
import numpy as np
import jax
import jax.numpy as jnp
from jax import lax
from jax.experimental import pallas as pl
from jax.experimental.pallas import tpu as pltpu
from jax.sharding import PartitionSpec as P

NORM_EPS = 1e-5
GROUP_EPS = 1e-6
ROPE_BASE = 10000.0
BF = jnp.bfloat16
F32 = jnp.float32
MESH = pl.DeviceIdType.MESH
SLOTS = 4


def layer_norm(x_f32, norm_gain, norm_bias):
    row_mean = jnp.mean(x_f32, axis=-1, keepdims=True)
    centered = x_f32 - row_mean
    variance = jnp.mean(centered * centered, axis=-1, keepdims=True)
    return centered * lax.rsqrt(variance + NORM_EPS) * norm_gain + norm_bias


def rope_constants(chunk_len, key_dim):
    half_dim = key_dim // 2
    inv_freq = np.power(ROPE_BASE, -np.arange(half_dim) / half_dim).astype(np.float32)
    step_angles = np.arange(chunk_len)[:, None] * inv_freq.astype(np.float64)[None, :]
    return jnp.asarray(inv_freq[None, :]), jnp.asarray(np.cos(step_angles).astype(np.float32)), jnp.asarray(np.sin(step_angles).astype(np.float32))


def split2(val):
    high = val.astype(BF)
    return high, (val - high.astype(F32)).astype(BF)


def dot(lhs, rhs):
    return jnp.dot(lhs, rhs, preferred_element_type=F32)


def ln_rows(load, store, g_ref, b_ref, width):
    cols = [slice(c, c + 256) for c in range(0, width, 256)]
    total = load(cols[0])
    for col in cols[1:]:
        total = total + load(col)
    mean = jnp.sum(total, axis=-1, keepdims=True) * (1.0 / width)
    total = None
    for col in cols:
        cent = load(col) - mean
        total = cent * cent if total is None else total + cent * cent
    var = jnp.sum(total, axis=-1, keepdims=True) * (1.0 / width)
    scale = lax.rsqrt(var + NORM_EPS)
    for col in cols:
        store(col, ((load(col) - mean) * scale * g_ref[:, col] + b_ref[:, col]).astype(BF))


def mix_kernel(lg_hbm, pos_hbm, x_hbm, freq_hbm, stepc_hbm, steps_hbm, g_hbm, b_hbm, wq, wk, wv, wg, s_hbm, z_hbm, so_hbm,
               lg_ref, pos_ref, freq_ref, stepc_ref, steps_ref, g_ref, b_ref, small_sem, cos_ref, sin_ref, xb, hb, wb, sb, sob, qb, kb, vb, gb, scb, sth, stl, kdb, ob, zb, xsem, wsem, ssem, sosem, zsem):
    heads = wq.shape[1] // 256
    nseq = s_hbm.shape[0]
    clen = x_hbm.shape[0] // nseq
    first_head = lax.axis_index('tp') * heads

    def wcopies(head, i):
        slot = lax.rem(head * 3 + i, SLOTS)
        wide = pl.ds(pl.multiple_of(head * 512, 512), 512)
        narrow = pl.ds(pl.multiple_of(head * 256, 256), 256)
        if i == 0:
            return (pltpu.make_async_copy(wq.at[:, narrow], wb.at[slot, :, :256], wsem.at[slot, 0]),
                    pltpu.make_async_copy(wk.at[:, narrow], wb.at[slot, :, 256:], wsem.at[slot, 1]))
        return (pltpu.make_async_copy((wv if i == 1 else wg).at[:, wide], wb.at[slot], wsem.at[slot, 0]),)

    def wstart(head, i):
        for copy in wcopies(head, i):
            copy.start()

    def scopy(head):
        slot = lax.rem(head, 2)
        return pltpu.make_async_copy(s_hbm.at[:, head], sb.at[slot], ssem.at[slot])

    def socopy(head, s):
        slot = lax.rem(head, 2)
        return pltpu.make_async_copy(sob.at[slot, s], so_hbm.at[s, head], sosem.at[slot, s])

    def so_wait(head):
        for s in range(nseq):
            socopy(head, s).wait()

    def zcopy(head):
        slot = lax.rem(head, 2)
        return pltpu.make_async_copy(zb.at[slot], z_hbm.at[:, pl.ds(pl.multiple_of(head * 512, 512), 512)], zsem.at[slot])

    def xcopy(s):
        rows = pl.ds(pl.multiple_of(s * clen, clen), clen)
        return pltpu.make_async_copy(x_hbm.at[rows], xb.at[rows], xsem.at[s])

    small = ((pos_hbm, pos_ref), (freq_hbm, freq_ref), (stepc_hbm, stepc_ref), (steps_hbm, steps_ref),
             (g_hbm, g_ref), (b_hbm, b_ref), (lg_hbm, lg_ref))
    small = [pltpu.make_async_copy(src, dst, small_sem.at[i]) for i, (src, dst) in enumerate(small)]
    for copy in small:
        copy.start()
    for s in range(nseq):
        xcopy(s).start()
    wstart(0, 0)
    for copy in small:
        copy.wait()

    def ln_body(s, carry):
        xcopy(s).wait()

        @pl.when(s == nseq - 1)
        def _():
            for i in range(1, SLOTS):
                wstart(i // 3, i % 3)
            scopy(0).start()
            scopy(1).start()
        rows = pl.ds(pl.multiple_of(s * clen, clen), clen)

        def store(col, val):
            hb[rows, col] = val
        ln_rows(lambda col: xb[rows, col].astype(F32), store, g_ref, b_ref, xb.shape[1])
        return carry
    def rope_body(s, carry):
        angle = pos_ref[s].astype(F32) * freq_ref[...]
        base_c, base_s = jnp.cos(angle), jnp.sin(angle)
        rows = pl.ds(pl.multiple_of(s * clen, clen), clen)
        cos_ref[rows, :] = base_c * stepc_ref[...] - base_s * steps_ref[...]
        sin_ref[rows, :] = base_s * stepc_ref[...] + base_c * steps_ref[...]
        return carry
    lax.fori_loop(0, nseq, rope_body, 0)

    lax.fori_loop(0, nseq, ln_body, 0)

    step_i = lax.broadcasted_iota(jnp.int32, (clen, clen), 0)
    step_j = lax.broadcasted_iota(jnp.int32, (clen, clen), 1)
    gap = step_i - step_j
    tok_q = lax.broadcasted_iota(jnp.int32, (clen, 512), 0).astype(F32)
    tok_k = lax.broadcasted_iota(jnp.int32, (clen, 256), 0).astype(F32)

    def project(head, i):
        return dot(hb[...], wb[lax.rem(head * 3 + i, SLOTS)])

    def wwait(head, i):
        for copy in wcopies(head, i):
            copy.wait()

    def wnext(head, i):
        next_head, next_i = head + (i + SLOTS) // 3, (i + SLOTS) % 3

        @pl.when(next_head < heads)
        def _():
            wstart(next_head, next_i)

    def proj_qk(head, slot):
        cos_t = cos_ref[...]
        sin_t = sin_ref[...]
        qk = project(head, 0)
        q, k = qk[:, :256], qk[:, 256:]
        qb[slot, :, :128] = (q[:, :128] * cos_t - q[:, 128:] * sin_t).astype(BF)
        qb[slot, :, 128:] = (q[:, 128:] * cos_t + q[:, :128] * sin_t).astype(BF)
        kb[slot, :, :128] = ((k[:, :128] * cos_t - k[:, 128:] * sin_t) * 0.0625).astype(BF)
        kb[slot, :, 128:] = ((k[:, 128:] * cos_t + k[:, :128] * sin_t) * 0.0625).astype(BF)

    def proj_v(head, slot):
        val = project(head, 1).astype(BF)
        for s in range(nseq):
            for copy in range(2):
                vb[slot, s, copy * clen:(copy + 1) * clen, :] = val[s * clen:(s + 1) * clen]

    def proj_g(head, slot):
        gb[slot] = project(head, 2)

    def seq_rows(s):
        return slice(s * clen, (s + 1) * clen)

    def ret_scores(slot):
        return [lax.dot_general(qb[slot, seq_rows(s), :], kb[slot, seq_rows(s), :], (((1,), (1,)), ((), ())),
                                preferred_element_type=F32) for s in range(nseq)]

    def ret_prepare(head, slot, scores):
        log_g = lg_ref[first_head + head]
        inner_decay = jnp.where(gap >= 0, jnp.exp(jnp.maximum(gap, 0).astype(F32) * log_g), 0.0)
        key_decay = jnp.exp((clen - 1.0 - tok_k) * log_g)
        for s in range(nseq):
            sth[s], stl[s] = split2(sb[slot, s])
            kdb[s, :clen], kdb[s, clen:] = split2(kb[slot, seq_rows(s), :].astype(F32) * key_decay)
            high, low = split2(scores[s] * inner_decay)
            scb[s] = jnp.concatenate([high, low], axis=-1)

    def ret_out(head, slot, early=False):
        log_g = lg_ref[first_head + head]
        query_decay = jnp.exp((tok_q + 1.0) * log_g)
        state_decay = jnp.exp(jnp.full((1, 512), clen, F32) * log_g)
        for s in range(nseq):
            q = qb[slot, seq_rows(s), :]
            ob[seq_rows(s), :] = dot(scb[s], vb[slot, s]) + (dot(q, sth[s]) + dot(q, stl[s])) * query_decay
            update = lax.dot_general(kdb[s], vb[slot, s], (((0,), (0,)), ((), ())), preferred_element_type=F32)
            sob[slot, s] = sb[slot, s] * state_decay + update
            if early:
                socopy(head, s).start()

    def ret_gate(slot):
        for s in range(nseq):
            out = ob[seq_rows(s), :]
            mean = jnp.mean(out, axis=-1, keepdims=True)
            cent = out - mean
            var = jnp.mean(cent * cent, axis=-1, keepdims=True)
            gates = gb[slot, seq_rows(s), :]
            zb[slot, seq_rows(s), :] = (gates * jax.nn.sigmoid(gates) * (cent * lax.rsqrt(var + GROUP_EPS))).astype(BF)

    wwait(0, 0)
    proj_qk(0, 0)
    wnext(0, 0)
    wwait(0, 1)
    proj_v(0, 0)
    wnext(0, 1)
    wwait(0, 2)
    proj_g(0, 0)
    wnext(0, 2)

    def head_body(head, carry):
        prev = head - 1
        slot = lax.rem(head, 2)
        old = 1 - slot
        scopy(prev).wait()

        @pl.when(prev >= 2)
        def _():
            so_wait(prev - 2)
            zcopy(prev - 2).wait()
        wwait(head, 0)
        scores = ret_scores(old)
        proj_qk(head, slot)
        ret_prepare(prev, old, scores)
        wnext(head, 0)
        wwait(head, 1)
        ret_out(prev, old)
        proj_v(head, slot)
        wnext(head, 1)
        for s in range(nseq):
            socopy(prev, s).start()

        @pl.when(head + 1 < heads)
        def _():
            scopy(head + 1).start()
        wwait(head, 2)
        proj_g(head, slot)
        ret_gate(old)
        wnext(head, 2)
        zcopy(prev).start()
        return carry

    lax.fori_loop(1, heads, head_body, 0)
    last = heads - 1
    slot = last % 2
    scopy(last).wait()
    so_wait(last - 2)
    zcopy(last - 2).wait()
    ret_prepare(last, slot, ret_scores(slot))
    ret_out(last, slot, early=True)
    ret_gate(slot)
    zcopy(last).start()
    for head in (last - 1, last):
        so_wait(head)
        zcopy(head).wait()


def mix_call(x2d, start_pos, gain, bias, w_q, w_k, w_v, w_g, state, log_gammas):
    rows, d_model = x2d.shape
    nseq, heads = state.shape[:2]
    clen = rows // nseq
    anyspec = pl.BlockSpec(memory_space=pl.ANY)
    return pl.pallas_call(
        mix_kernel,
        out_shape=(jax.ShapeDtypeStruct((rows, heads * 512), BF), jax.ShapeDtypeStruct(state.shape, F32)),
        in_specs=[anyspec] * 13,
        out_specs=(anyspec, anyspec),
        scratch_shapes=[
            pltpu.SMEM(log_gammas.shape, F32), pltpu.SMEM(start_pos.shape, jnp.int32),
            pltpu.VMEM((1, 128), F32), pltpu.VMEM((clen, 128), F32), pltpu.VMEM((clen, 128), F32),
            pltpu.VMEM((1, d_model), F32), pltpu.VMEM((1, d_model), F32), pltpu.SemaphoreType.DMA((7,)),
            pltpu.VMEM((rows, 128), F32), pltpu.VMEM((rows, 128), F32),
            pltpu.VMEM((rows, d_model), BF), pltpu.VMEM((rows, d_model), BF),
            pltpu.VMEM((SLOTS, d_model, 512), BF),
            pltpu.VMEM((2, nseq, 256, 512), F32), pltpu.VMEM((2, nseq, 256, 512), F32),
            pltpu.VMEM((2, rows, 256), BF), pltpu.VMEM((2, rows, 256), BF), pltpu.VMEM((2, nseq, 2 * clen, 512), BF),
            pltpu.VMEM((2, rows, 512), F32),
            pltpu.VMEM((nseq, clen, 2 * clen), BF), pltpu.VMEM((nseq, 256, 512), BF), pltpu.VMEM((nseq, 256, 512), BF),
            pltpu.VMEM((nseq, 2 * clen, 256), BF), pltpu.VMEM((rows, 512), F32), pltpu.VMEM((2, rows, 512), BF),
            pltpu.SemaphoreType.DMA((nseq,)), pltpu.SemaphoreType.DMA((SLOTS, 2)), pltpu.SemaphoreType.DMA((2,)),
            pltpu.SemaphoreType.DMA((2, nseq)), pltpu.SemaphoreType.DMA((2,)),
        ],
        compiler_params=pltpu.CompilerParams(vmem_limit_bytes=60 * 1024 * 1024),
        cost_estimate=pl.CostEstimate(flops=21_000_000_000, bytes_accessed=102_000_000, transcendentals=0),
        name='mix',
    )(log_gammas, start_pos, x2d, *rope_constants(clen, state.shape[2]), gain, bias, w_q, w_k, w_v, w_g, state)


TN = 512


def ffn_kernel(z_hbm, x_hbm, g_hbm, b_hbm, wo, wup, wdn, o_hbm,
               g_ref, b_ref, gb_sem, zb, wa, wbb, ub, drv, xrv, h2, x1,
               zsem, x1sem, wosem, wupsem, wdnsem, ds_sem, dr_sem, xs_sem, xr_sem, hs_sem, hr_sem, ol_sem, os_sem, or_sem):
    tp = lax.axis_index('tp')
    core = lax.rem(tp, 2)
    sib = {'tp': tp + 1 - 2 * core}
    nbr = {'tp': lax.rem(tp + 2, 4)}
    nt = wo.shape[1] // TN
    ku = wup.shape[1] // 256
    hrows = ub.shape[2]

    def wo_copy(n):
        return pltpu.make_async_copy(wo.at[:, pl.ds(pl.multiple_of(n * TN, TN), TN)], wbb.at[n], wosem.at[n])

    def wdn_copy(n):
        return pltpu.make_async_copy(wdn.at[:, pl.ds(pl.multiple_of(n * TN, TN), TN)], wbb.at[n], wdnsem.at[n])

    def wup_copy(n):
        return pltpu.make_async_copy(wup.at[:, pl.ds(pl.multiple_of(n * 256, 256), 256)], wa.at[n], wupsem.at[n])

    def x1_copy(c):
        src = x_hbm.at[pl.ds(pl.multiple_of((c * 2 + core) * hrows, hrows), hrows)]
        return pltpu.make_async_copy(src, x1.at[c], x1sem.at[c])

    zcopy = pltpu.make_async_copy(z_hbm, zb, zsem)
    zcopy.start()

    def start_wo(n, carry):
        wo_copy(n).start()
        return carry
    lax.fori_loop(0, nt, start_wo, 0)
    gain_copies = (pltpu.make_async_copy(g_hbm, g_ref, gb_sem.at[0]), pltpu.make_async_copy(b_hbm, b_ref, gb_sem.at[1]))
    for copy in gain_copies:
        copy.start(priority=1)
    x1_copy(0).start(priority=1)
    x1_copy(1).start(priority=1)

    def start_wup(n, carry):
        wup_copy(n).start(priority=1)
        return carry
    lax.fori_loop(0, ku, start_wup, 0)

    barrier = pltpu.get_barrier_semaphore()
    pl.semaphore_signal(barrier, inc=1, device_id=sib, device_id_type=MESH)
    pl.semaphore_signal(barrier, inc=1, device_id=nbr, device_id_type=MESH)
    pl.semaphore_wait(barrier, 2)

    def d_copy(r, c, n):
        return pltpu.make_async_remote_copy(
            src_ref=ub.at[c * 2 + 1 - core, n], dst_ref=drv.at[c, n], send_sem=ds_sem.at[r, c, n], recv_sem=dr_sem.at[r, c, n],
            device_id=sib, device_id_type=MESH)

    def x_copy(r, c, n):
        return pltpu.make_async_remote_copy(
            src_ref=ub.at[c * 2 + core, n], dst_ref=xrv.at[r, c, n], send_sem=xs_sem.at[r, c, n], recv_sem=xr_sem.at[r, c, n],
            device_id=nbr, device_id_type=MESH)

    def forward(r, c, n):
        d_copy(r, c, n).wait_recv()
        own = ub[c * 2 + core, n].astype(F32)
        ub[c * 2 + core, n] = (own + drv[c, n].astype(F32)).astype(BF)
        x_copy(r, c, n).start()

    lag = 2
    zcopy.wait()

    def wo_step(n, carry):
        wo_copy(n).wait()
        res = dot(zb[...], wbb[n]).astype(BF)
        for j in range(4):
            ub[j, n] = res[j * hrows:(j + 1) * hrows]
        d_copy(0, 0, n).start()
        d_copy(0, 1, n).start()
        wdn_copy(n).start(priority=1)

        @pl.when(n >= 1)
        def _():
            forward(0, 0, n - 1)
        return carry
    lax.fori_loop(0, nt, wo_step, 0)
    forward(0, 0, nt - 1)

    def fwd1(n, carry):
        forward(0, 1, n)
        return carry
    lax.fori_loop(0, nt, fwd1, 0)

    def h_copy(c):
        own = h2.at[c, pl.ds(pl.multiple_of(core * hrows, hrows), hrows)]
        return pltpu.make_async_remote_copy(src_ref=own, dst_ref=own, send_sem=hs_sem.at[c], recv_sem=hr_sem.at[c],
                                            device_id=sib, device_id_type=MESH)

    def chunk(c):
        x1_copy(c).wait()
        for n in range(nt):
            x_copy(0, c, n).wait_recv()

        def ln_rows(r, carry):
            rows = pl.ds(pl.multiple_of(r * 16, 16), 16)
            total = jnp.concatenate(
                [(ub[c * 2 + core, n, rows, :].astype(F32) + xrv[0, c, n, rows, :].astype(F32)).astype(BF) for n in range(nt)], axis=-1)
            mid = (x1[c, rows, :].astype(F32) + total.astype(F32)).astype(BF)
            x1[c, rows, :] = mid
            hrow = pl.ds(pl.multiple_of(core * hrows + r * 16, 16), 16)
            h2[c, hrow, :] = layer_norm(mid.astype(F32), g_ref[...], b_ref[...]).astype(BF)
            return carry
        lax.fori_loop(0, hrows // 16, ln_rows, 0)
        h_copy(c).start()

        def drain(n, carry):
            d_copy(0, c, n).wait_send()
            x_copy(0, c, n).wait_send()
            return carry
        lax.fori_loop(0, nt, drain, 0)
        h_copy(c).wait_recv()

        def up_step(n, carry):
            if c == 0:
                wup_copy(n).wait()
            res = dot(h2[c], wa[n])
            res = 0.5 * res * (1.0 + lax.erf(res * (0.5 ** 0.5)))
            zb[c * 2 * hrows:(c + 1) * 2 * hrows, pl.ds(pl.multiple_of(n * 256, 256), 256)] = res.astype(BF)
            return carry
        lax.fori_loop(0, ku, up_step, 0)

        def down_step(n, carry):
            if c == 0:
                wdn_copy(n).wait()
            res = dot(zb[c * 2 * hrows:(c + 1) * 2 * hrows, :], wbb[n]).astype(BF)
            for j in range(2):
                ub[c * 2 + j, n] = res[j * hrows:(j + 1) * hrows]
            d_copy(1, c, n).start()

            @pl.when(n >= lag)
            def _():
                forward(1, c, n - lag)
            return carry
        lax.fori_loop(0, nt, down_step, 0)
        for n in range(nt - lag, nt):
            forward(1, c, n)

    for copy in gain_copies:
        copy.wait()
    chunk(0)
    chunk(1)

    def o_copies(c, n):
        src = x1.at[c, :, pl.ds(pl.multiple_of(n * TN, TN), TN)]
        dst = o_hbm.at[pl.ds(pl.multiple_of((c * 2 + core) * hrows, hrows), hrows), pl.ds(pl.multiple_of(n * TN, TN), TN)]
        local = pltpu.make_async_copy(src, dst, ol_sem.at[c, n])
        remote = pltpu.make_async_remote_copy(src_ref=src, dst_ref=dst, send_sem=os_sem.at[c, n], recv_sem=or_sem.at[c, n],
                                              device_id=sib, device_id_type=MESH)
        return local, remote

    for c in range(2):
        def out_step(n, carry):
            x_copy(1, c, n).wait_recv()
            cols = pl.ds(pl.multiple_of(n * TN, TN), TN)
            total = (ub[c * 2 + core, n].astype(F32) + xrv[1, c, n].astype(F32)).astype(BF)
            x1[c, :, cols] = (x1[c, :, cols].astype(F32) + total.astype(F32)).astype(BF)
            local, remote = o_copies(c, n)
            remote.start()
            local.start()
            return carry
        lax.fori_loop(0, nt, out_step, 0)
    for c in range(2):
        h_copy(c).wait_send()

        def fin(n, carry):
            d_copy(1, c, n).wait_send()
            x_copy(1, c, n).wait_send()
            local, remote = o_copies(c, n)
            local.wait()
            remote.wait_send()
            remote.wait_recv()
            return carry
        lax.fori_loop(0, nt, fin, 0)


def ffn_call(z2d, x2d, gain, bias, w_o, w_up, w_down):
    rows, d_model = x2d.shape
    width = z2d.shape[1]
    fdim = w_up.shape[1]
    nt = d_model // TN
    ku = fdim // 256
    hr = rows // 4
    anyspec = pl.BlockSpec(memory_space=pl.ANY)
    dma = pltpu.SemaphoreType.DMA
    return pl.pallas_call(
        ffn_kernel,
        out_shape=jax.ShapeDtypeStruct((rows, d_model), BF),
        in_specs=[anyspec] * 7,
        out_specs=anyspec,
        scratch_shapes=[
            pltpu.VMEM((1, d_model), F32), pltpu.VMEM((1, d_model), F32), dma((2,)),
            pltpu.VMEM((rows, width), BF),
            pltpu.VMEM((ku, d_model, 256), BF),
            pltpu.VMEM((nt, width, TN), BF),
            pltpu.VMEM((4, nt, hr, TN), BF),
            pltpu.VMEM((2, nt, hr, TN), BF),
            pltpu.VMEM((2, 2, nt, hr, TN), BF),
            pltpu.VMEM((2, 2 * hr, d_model), BF),
            pltpu.VMEM((2, hr, d_model), BF),
            dma, dma((2,)), dma((nt,)), dma((ku,)), dma((nt,)),
            dma((2, 2, nt)), dma((2, 2, nt)), dma((2, 2, nt)), dma((2, 2, nt)), dma((2,)), dma((2,)),
            dma((2, nt)), dma((2, nt)), dma((2, nt)),
        ],
        compiler_params=pltpu.CompilerParams(collective_id=0, has_side_effects=True, vmem_limit_bytes=67043328),
        cost_estimate=pl.CostEstimate(flops=20_000_000_000, bytes_accessed=85_000_000, transcendentals=0),
        name='ffn',
    )(z2d, x2d, gain, bias, w_o, w_up, w_down)


def emit_kernel(src, dst, buf, in_sem, out_sem):
    parts = buf.shape[0]
    ins = [pltpu.make_async_copy(src.at[i], buf.at[i], in_sem.at[i]) for i in range(parts)]
    outs = [pltpu.make_async_copy(buf.at[i], dst.at[i], out_sem.at[i]) for i in range(parts)]
    for copy in ins:
        copy.start()
    for copy_in, copy_out in zip(ins, outs):
        copy_in.wait()
        copy_out.start()
    for copy in outs:
        copy.wait()


def emit_call(out):
    dma = pltpu.SemaphoreType.DMA
    anyspec = pl.BlockSpec(memory_space=pl.ANY)
    return pl.pallas_call(
        emit_kernel, out_shape=jax.ShapeDtypeStruct(out.shape, out.dtype), in_specs=[anyspec], out_specs=anyspec,
        scratch_shapes=[pltpu.VMEM(out.shape, out.dtype), dma((out.shape[0],)), dma((out.shape[0],))],
        compiler_params=pltpu.CompilerParams(vmem_limit_bytes=60 * 1024 * 1024),
        name='emit',
    )(out)


def solution(mesh):
    def local_layer(x_in, start_pos, kv_state, ln1_gain, ln1_bias, w_q, w_k, w_v, w_g, w_o, ln2_gain, ln2_bias, w_up, w_down):
        nseq, clen, d_model = x_in.shape
        x2d = x_in.reshape(nseq * clen, d_model)
        num_heads = kv_state.shape[1] * mesh.shape['tp']
        log_gammas = jnp.asarray(np.log1p(-np.exp2(-5.0 - np.arange(num_heads))).astype(np.float32))
        z2d, new_state = mix_call(x2d, start_pos, ln1_gain.reshape(1, -1), ln1_bias.reshape(1, -1),
                                  w_q, w_k, w_v, w_g, kv_state, log_gammas)
        out = ffn_call(z2d, x2d, ln2_gain.reshape(1, -1), ln2_bias.reshape(1, -1), w_o, w_up, w_down)
        return emit_call(out.reshape(8, -1, d_model)).reshape(x_in.shape), new_state

    in_specs = (P('dp', None, None), P('dp'), P('dp', 'tp', None, None), P(), P(), P(None, 'tp'), P(None, 'tp'), P(None, 'tp'), P(None, 'tp'), P('tp', None), P(), P(), P(None, 'tp'), P('tp', None))
    out_specs = (P('dp', None, None), P('dp', 'tp', None, None))
    return jax.shard_map(local_layer, mesh=mesh, in_specs=in_specs, out_specs=out_specs, check_vma=False)
```
